512 devices in a mesh: dp: 32 (over y, x), mp: 16 (over z, core).
Axes of the slice: x: 4, y: 8, z: 8, core: 2. Of those that a mesh axis runs over, the one named last changes fastest.
Arguments:
- query_new: bfloat16 [512, 4096], P(('dp', 'mp')), parts along dimension 0, may hold values from -140 to 140
- key_new: bfloat16 [512, 1024], P(('dp', 'mp')), parts along dimension 0, may hold values from -5 to 5
- value_new: bfloat16 [512, 1024], P(('dp', 'mp')), parts along dimension 0, may hold values from -5 to 5
- prefix_keys: bfloat16 [65536, 1024], P(('dp', 'mp')), parts along dimension 0, may hold values from -5 to 5
- prefix_values: bfloat16 [65536, 1024], P(('dp', 'mp')), parts along dimension 0, may hold values from -5 to 5
- sample_suffix_keys: bfloat16 [512, 64, 1024], P(('dp', 'mp')), parts along dimension 0, may hold values from -5 to 5
- sample_suffix_values: bfloat16 [512, 64, 1024], P(('dp', 'mp')), parts along dimension 0, may hold values from -5 to 5
- prefix_len: int32 [32], P('dp'), parts along dimension 0, may hold values from 512 to 2048
- suffix_len: int32 [512], P(('dp', 'mp')), parts along dimension 0, may hold values from 1 to 64, as said below
- residual: bfloat16 [512, 8192], P(('dp', 'mp')), parts along dimension 0, may hold values from -3 to 3
- out_weight: bfloat16 [4096, 8192], P('mp'), may hold values from -0.1875 to 0.1875
- norm_gain: bfloat16 [8192], replicated, may hold values from 0.5 to 1.5
Outputs:
- hidden: bfloat16 [512, 8192], P(('dp', 'mp')), parts along dimension 0
- normed: bfloat16 [512, 8192], P(('dp', 'mp')), parts along dimension 0
The draws below stay inside these ranges and needn't reach their ends.
There are 32 independent parts, one for each index of `dp`. The reference program is written for one: setup_inputs(seed, part) draws one part's arguments, and reference() takes and returns one part's arrays. A program takes and returns all parts, laid end to end along the dimension named above; an argument that names none is the same for every part. Nothing has to cross between parts.
Inputs may be any that keep to these rules, and one draw needn't show every extreme that they name: `suffix_len`: some sample has exactly 64 cached generated tokens.
All inputs are finite; a program needn't handle non-finite values.
Results may differ from the reference program's by a relative error of at most 0.0085.
Values may be sent and summed in bfloat16 or wider, within the bound.
No kernel may reach another device: no remote copies, remote signals or barrier semaphores. Data moves between devices by JAX's collectives and lax.ppermute only.
A program may use at most 64 MiB of HBM per device.

```python
import jax
import jax.numpy as jnp
from jax import lax

D = 8192
HEAD_SIZE = 128
KEY_VALUE_HEADS = 8
HQ = 32
SUFFIX_POSITIONS = 64
SAMPLE_COUNT = 16
PRE = 2048


def joint_keys_queries(key):
    base = jax.random.fold_in(key, 7)
    keys = jnp.clip(jax.random.normal(jax.random.fold_in(base, 1), (PRE, KEY_VALUE_HEADS * HEAD_SIZE), jnp.float32), -5.0, 5.0)
    queries = jnp.clip(2.0 * jax.random.normal(jax.random.fold_in(base, 2), (SAMPLE_COUNT, HQ * HEAD_SIZE), jnp.float32), -8.0, 8.0)
    return (keys, queries)


def draw_prefix_keys(key, part):
    keys, queries = joint_keys_queries(key)
    return keys.astype(jnp.bfloat16)


def draw_query_new(key, part):
    keys, queries = joint_keys_queries(key)
    return queries.astype(jnp.bfloat16)


def draw_suffix_len(key, part):
    base = jax.random.fold_in(key, 31)
    lengths = jax.random.randint(jax.random.fold_in(base, 1), (SAMPLE_COUNT,), 1, SUFFIX_POSITIONS + 1, dtype=jnp.int32)
    chosen = jax.random.randint(jax.random.fold_in(base, 2), (), 0, SAMPLE_COUNT, dtype=jnp.int32)
    lengths = jnp.where(jnp.arange(SAMPLE_COUNT, dtype=jnp.int32) == chosen, SUFFIX_POSITIONS, lengths)
    return lengths.astype(jnp.int32)


def block_levels(stream_key, shape, pieces, low, top_value):
    factor_of, own = 1.0, jax.random.fold_in(stream_key, 6)
    for axis_at, blocks in pieces:
        heights = jnp.exp(jax.random.uniform(jax.random.fold_in(own, axis_at), (blocks,), jnp.float32, low / len(pieces), top_value / len(pieces)))
        factor_of = factor_of * jnp.repeat(heights, shape[axis_at] // blocks).reshape([-1 if axis == axis_at else 1 for axis in range(len(shape))])
    return factor_of


def centred(own_key, shape, deviation, limit, split=(), kind=jnp.bfloat16):
    array = jax.random.normal(own_key, shape, jnp.float32) * deviation
    if len(split) > 0:
        array = block_levels(own_key, shape, split, -0.22, 0.18) * array
    return jnp.clip(array, min=-limit, max=limit).astype(kind)


def setup_inputs(seed: int = 0, part: int = 0) -> dict:
    arg_keys = jax.random.split(jax.random.key(seed), 13)
    part_keys = jax.random.split(jax.random.fold_in(arg_keys[12], part), 13)
    return {
        "query_new": draw_query_new(jax.random.fold_in(jax.random.fold_in(arg_keys[12], part), 71), part),
        "key_new": centred(part_keys[1], (SAMPLE_COUNT, KEY_VALUE_HEADS * HEAD_SIZE), 1.0, 5.0, ((0, 16),)),
        "value_new": centred(part_keys[2], (SAMPLE_COUNT, KEY_VALUE_HEADS * HEAD_SIZE), 1.0, 5.0, ((0, 16),)),
        "prefix_keys": draw_prefix_keys(jax.random.fold_in(jax.random.fold_in(arg_keys[12], part), 71), part),
        "prefix_values": centred(part_keys[4], (PRE, KEY_VALUE_HEADS * HEAD_SIZE), 1.0, 5.0, ((0, 16),)),
        "sample_suffix_keys": centred(part_keys[5], (SAMPLE_COUNT, SUFFIX_POSITIONS, KEY_VALUE_HEADS * HEAD_SIZE), 1.0, 5.0, ((0, 16),)),
        "sample_suffix_values": centred(part_keys[6], (SAMPLE_COUNT, SUFFIX_POSITIONS, KEY_VALUE_HEADS * HEAD_SIZE), 1.0, 5.0, ((0, 16),)),
        "prefix_len": jax.random.randint(part_keys[7], (1,), PRE // 4, PRE + 1).astype(jnp.int32),
        "suffix_len": draw_suffix_len(jax.random.fold_in(jax.random.fold_in(arg_keys[12], part), 71), part),
        "residual": centred(part_keys[9], (SAMPLE_COUNT, D), 0.5, 3.0, ((0, 16),)),
        "out_weight": centred(arg_keys[10], (HQ * HEAD_SIZE, D), (HQ * HEAD_SIZE // 4) ** -0.5, 0.1875, ((0, 16),)),
        "norm_gain": jnp.clip(1.0 + 0.1 * jax.random.normal(arg_keys[11], (D,), jnp.float32), 0.5, 1.5).astype(jnp.bfloat16),
    }


def reference(query_new, key_new, value_new, prefix_keys, prefix_values, sample_suffix_keys, sample_suffix_values, prefix_len, suffix_len, residual, out_weight, norm_gain):
    group = HQ // KEY_VALUE_HEADS
    score_scale = HEAD_SIZE ** (-0.5)
    query_vector = query_new.astype(jnp.float32).reshape(SAMPLE_COUNT, KEY_VALUE_HEADS, group, HEAD_SIZE)
    pkeys = prefix_keys.astype(jnp.float32).reshape(PRE, KEY_VALUE_HEADS, HEAD_SIZE)
    prefix_value_rows = prefix_values.astype(jnp.float32).reshape(PRE, KEY_VALUE_HEADS, HEAD_SIZE)
    suffix_key_rows = sample_suffix_keys.astype(jnp.float32).reshape(SAMPLE_COUNT, SUFFIX_POSITIONS, KEY_VALUE_HEADS, HEAD_SIZE)
    suffix_value_rows = sample_suffix_values.astype(jnp.float32).reshape(SAMPLE_COUNT, SUFFIX_POSITIONS, KEY_VALUE_HEADS, HEAD_SIZE)
    fresh_key_rows = key_new.astype(jnp.float32).reshape(SAMPLE_COUNT, KEY_VALUE_HEADS, HEAD_SIZE)
    nvals = value_new.astype(jnp.float32).reshape(SAMPLE_COUNT, KEY_VALUE_HEADS, HEAD_SIZE)
    pvalid = jnp.arange(PRE, dtype=jnp.int32) < prefix_len[0]
    svalid = jnp.arange(SUFFIX_POSITIONS, dtype=jnp.int32)[None, :] < suffix_len[:, None]
    s_pre = jnp.einsum('bkgd,pkd->bkgp', query_vector, pkeys) * score_scale
    suffix_score_rows = jnp.einsum('cqxt,caqt->cqxa', query_vector, suffix_key_rows) * score_scale
    fresh_score_rows = jnp.einsum('exio,exo->exi', query_vector, fresh_key_rows) * score_scale
    s_pre = jnp.where(pvalid[None, None, None, :], s_pre, -jnp.inf)
    suffix_score_rows = jnp.where(svalid[:, None, None, :], suffix_score_rows, -jnp.inf)
    top = jnp.maximum(jnp.maximum(lax.optimization_barrier(jnp.max(s_pre, -1)), lax.optimization_barrier(jnp.max(suffix_score_rows, -1))), fresh_score_rows)
    w_pre = jnp.exp(s_pre - top[..., None])
    suffix_weight_rows = jnp.exp(suffix_score_rows - top[..., None])
    w_new = jnp.exp(fresh_score_rows - top)
    total = lax.optimization_barrier(jnp.sum(w_pre, -1)) + lax.optimization_barrier(jnp.sum(suffix_weight_rows, -1)) + w_new
    prefix_bias_rows = w_pre.astype(jnp.bfloat16).astype(jnp.float32)
    suffix_bias_rows = suffix_weight_rows.astype(jnp.bfloat16).astype(jnp.float32)
    b_new = w_new.astype(jnp.bfloat16).astype(jnp.float32)
    summed_rows = jnp.einsum('wnso,onr->wnsr', prefix_bias_rows, prefix_value_rows) + jnp.einsum('cjax,cxjq->cjaq', suffix_bias_rows, suffix_value_rows)
    summed_rows = summed_rows + b_new[..., None] * nvals[:, :, None, :]
    attn = (summed_rows / total[..., None]).astype(jnp.bfloat16).reshape(SAMPLE_COUNT, HQ * HEAD_SIZE)
    proj = jnp.dot(attn, out_weight, preferred_element_type=jnp.float32)
    stream = residual.astype(jnp.float32) + proj
    hidden = stream.astype(jnp.bfloat16)
    meansq = lax.optimization_barrier(jnp.mean(stream * stream, axis=-1, keepdims=True))
    normed = (stream * jax.lax.rsqrt(meansq + 1e-05) * norm_gain.astype(jnp.float32)[None, :]).astype(jnp.bfloat16)
    return (hidden, normed)
```

```python
import functools

import jax
import jax.numpy as jnp
from jax import lax
from jax.experimental import pallas as pl
from jax.experimental.pallas import tpu as pltpu
from jax.sharding import PartitionSpec as P

HEAD_SIZE = 128
KEY_VALUE_HEADS = 8
HQ = 32
GROUP = HQ // KEY_VALUE_HEADS
SAMPLES = 16
CHIPS = 8
D = 8192
BLOCKS = D // 128
ROWS = 40
SCALE = HEAD_SIZE ** (-0.5)
MASKED = -1e30
LOWEST = -1e29
F32 = jnp.float32
BF16 = jnp.bfloat16


def vmem(count):
    return [pl.BlockSpec(memory_space=pltpu.VMEM)] * count


def at_most(mebibytes):
    return pltpu.CompilerParams(vmem_limit_bytes=mebibytes * 2**20)


def smem(count):
    return [pl.BlockSpec(memory_space=pltpu.SMEM)] * count


def spread_kernel(query_ref, out_ref):
    rows = [query_ref[0:1, h * 128 : (h + 1) * 128].astype(F32) for h in range(HQ)]
    rows = jnp.concatenate(rows, axis=0).astype(BF16)
    for i in range(SAMPLES):
        out_ref[i] = rows


def attend_kernel(
    place_ref,
    prefix_len_ref,
    suffix_len_ref,
    query_ref,
    pkeys_ref,
    pvalues_ref,
    skeys_ref,
    svalues_ref,
    key_ref,
    value_ref,
    out_ref,
    queries,
):
    place = place_ref[0]
    queries[...] = query_ref[...].reshape(SAMPLES * HQ, 128).astype(F32)
    row = lax.broadcasted_iota(jnp.int32, (64, 128), 0)
    lane = lax.broadcasted_iota(jnp.int32, (64, 128), 1)
    sample = 2 * (row % 8) + row // 32
    prefix_seen = lane + place * 128 < prefix_len_ref[0]
    own_seen = (sample == place) & ((lane < suffix_len_ref[0]) | (lane == 64))
    first = row == 0
    mark = lane[:32] == row[:32] + 32 * (place % 4)
    ones = jnp.ones((256, 128), BF16)
    zeros = jnp.zeros((5, 128), F32)
    for k in range(KEY_VALUE_HEADS):
        head = slice(k * 128, (k + 1) * 128)
        new_key = jnp.where(first, key_ref[0:1, head].astype(F32), 0.0).astype(BF16)
        new_value = jnp.where(first, value_ref[0:1, head].astype(F32), 0.0).astype(BF16)
        keys = jnp.concatenate([pkeys_ref[:, head], skeys_ref[0, :, head], new_key], axis=0)
        values = jnp.concatenate([pvalues_ref[:, head], svalues_ref[0, :, head], new_value], axis=0)
        query = [
            queries[pl.ds(c * HQ + k * GROUP + g, 8, stride=2 * HQ), :]
            for c in range(2)
            for g in range(GROUP)
        ]
        query = jnp.concatenate(query, axis=0).astype(BF16)
        scores = lax.dot_general(
            query, keys, (((1,), (1,)), ((), ())), preferred_element_type=F32
        )
        s_pre = jnp.where(prefix_seen, scores[:, :128] * SCALE, MASKED)
        s_own = jnp.where(own_seen, scores[:, 128:] * SCALE, MASKED)
        top = jnp.max(jnp.maximum(s_pre, s_own), axis=-1, keepdims=True)
        top = jnp.maximum(top, LOWEST).astype(BF16).astype(F32)
        weights = jnp.concatenate([jnp.exp(s_pre - top), jnp.exp(s_own - top)], axis=1)
        summed = jnp.dot(
            weights.astype(BF16),
            jnp.concatenate([values, ones], axis=1),
            preferred_element_type=F32,
        )
        total = summed[:, 128:]
        total_high = total.astype(BF16).astype(F32)
        total_low = total - total_high
        for c in range(2):
            part = slice(32 * c, 32 * c + 32)
            out_ref[2 * k + c, 0:32, :] = summed[part, :128].astype(BF16)
            stats = [
                jnp.sum(jnp.where(mark, v[part], 0.0), axis=0, keepdims=True)
                for v in (top, total_high, total_low)
            ]
            out_ref[2 * k + c, 32:ROWS, :] = jnp.concatenate(stats + [zeros], axis=0).astype(BF16)


def project_kernel(place_ref, got_ref, own_ref, other_ref, out_ref, rows):
    stats = got_ref[:, 32:ROWS, :].astype(F32)
    quads = [
        stats[4 * q] + stats[4 * q + 1] + stats[4 * q + 2] + stats[4 * q + 3] for q in range(4)
    ]
    tops = [s[0:1] for s in quads]
    totals = [s[1:2] + s[2:3] for s in quads]
    top = jnp.maximum(jnp.maximum(tops[0], tops[1]), jnp.maximum(tops[2], tops[3]))
    top = jnp.maximum(top, pltpu.roll(top, 64, 1))
    top = jnp.maximum(top, pltpu.roll(top, 32, 1))
    factors = [jnp.exp(t - top) for t in tops]
    total = sum(f * t for f, t in zip(factors, totals))
    total = total + pltpu.roll(total, 64, 1)
    total = total + pltpu.roll(total, 32, 1)
    row = lax.broadcasted_iota(jnp.int32, (32, 128), 0)
    lane = lax.broadcasted_iota(jnp.int32, (32, 128), 1)
    diagonal = lane % 32 == row
    mix = jnp.concatenate([jnp.where(diagonal, f / total, 0.0) for f in factors], axis=1)
    high = mix.astype(BF16)
    low = (mix - high.astype(F32)).astype(BF16)
    sums = got_ref[:, 0:32, :].reshape(SAMPLES * 32, 128)
    both = jnp.dot(jnp.concatenate([high, low], axis=0), sums, preferred_element_type=F32)
    attn = both[:32] + both[32:]
    attn = jnp.concatenate([attn[8 * g : 8 * g + 8] for g in range(GROUP)], axis=1)
    north = place_ref[0] % 2 == 1
    mine = jnp.where(north, attn[:, 256:], attn[:, :256]).astype(BF16)
    others = jnp.where(north, attn[:, :256], attn[:, 256:]).astype(BF16)
    width = 1024
    for n in range(0, D, width):
        cols = slice(n, n + width)
        piece = jnp.dot(mine, own_ref[:, cols], preferred_element_type=F32)
        piece += jnp.dot(others, other_ref[:, cols], preferred_element_type=F32)
        for i in range(width // 128):
            rows[pl.ds(n // 128 + i, 8, stride=BLOCKS), :] = piece[:, 128 * i : 128 * i + 128]
    out_ref[...] = rows[...].astype(BF16).reshape(CHIPS, BLOCKS, 128)


def finish_kernel(got_ref, residual_ref, gain_ref, hidden_ref, normed_ref):
    proj = got_ref[0].astype(F32)
    for i in range(1, CHIPS):
        proj += got_ref[i].astype(F32)
    stream = residual_ref[...].astype(F32) + proj
    hidden_ref[...] = stream.astype(BF16)
    scale = lax.rsqrt(jnp.sum(stream * stream) * (1.0 / D) + 1e-05)
    normed_ref[...] = (stream * scale * gain_ref[...].astype(F32)).astype(BF16)


def local(
    query_new,
    key_new,
    value_new,
    prefix_keys,
    prefix_values,
    sample_suffix_keys,
    sample_suffix_values,
    prefix_len,
    suffix_len,
    residual,
    out_weight,
    norm_gain,
):
    place = lax.axis_index("mp").astype(jnp.int32)[None]
    cores = [[2 * z + c for z in range(CHIPS)] for c in range(2)]
    other_weight = lax.ppermute(out_weight, "mp", [(i, i ^ 1) for i in range(SAMPLES)])
    spread = pl.pallas_call(
        spread_kernel,
        out_shape=jax.ShapeDtypeStruct((SAMPLES, HQ, 128), BF16),
        in_specs=vmem(1),
        out_specs=vmem(1)[0],
        compiler_params=at_most(2),
    )(query_new)
    queries = lax.all_to_all(spread, "mp", 0, 0, tiled=True)
    partial = pl.pallas_call(
        attend_kernel,
        out_shape=jax.ShapeDtypeStruct((SAMPLES, ROWS, 128), BF16),
        in_specs=smem(3) + vmem(7),
        out_specs=vmem(1)[0],
        scratch_shapes=[pltpu.VMEM((SAMPLES * HQ, 128), F32)],
        compiler_params=at_most(8),
    )(
        place,
        prefix_len,
        suffix_len,
        queries,
        prefix_keys,
        prefix_values,
        sample_suffix_keys,
        sample_suffix_values,
        key_new,
        value_new,
    )
    partial = lax.all_to_all(partial, "mp", 0, 0, tiled=True)
    proj = pl.pallas_call(
        project_kernel,
        out_shape=jax.ShapeDtypeStruct((CHIPS, BLOCKS, 128), BF16),
        in_specs=smem(1) + vmem(3),
        out_specs=vmem(1)[0],
        scratch_shapes=[pltpu.VMEM((8 * BLOCKS, 128), F32)],
        compiler_params=at_most(16),
    )(place, partial, out_weight, other_weight)
    proj = lax.all_to_all(proj, "mp", 0, 0, tiled=True, axis_index_groups=cores)
    hidden, normed = pl.pallas_call(
        finish_kernel,
        out_shape=[jax.ShapeDtypeStruct((BLOCKS, 128), BF16)] * 2,
        in_specs=vmem(3),
        out_specs=vmem(2),
        compiler_params=at_most(4),
    )(proj, residual.reshape(BLOCKS, 128), norm_gain.reshape(BLOCKS, 128))
    return hidden.reshape(1, D), normed.reshape(1, D)


def solution(mesh):
    whole = P(("dp", "mp"), None)
    placed = (
        whole,
        whole,
        whole,
        whole,
        whole,
        P(("dp", "mp"), None, None),
        P(("dp", "mp"), None, None),
        P("dp"),
        P(("dp", "mp")),
        whole,
        P("mp", None),
        P(),
    )
    return jax.shard_map(
        local, mesh=mesh, in_specs=placed, out_specs=(whole, whole), check_vma=False
    )
```

```python
import jax
import jax.numpy as jnp
from jax import lax
from jax.experimental import pallas as pl
from jax.experimental.pallas import tpu as pltpu
from jax.sharding import PartitionSpec as P


HEAD_SIZE = 128
KEY_VALUE_HEADS = 8
HQ = 32
GROUP = HQ // KEY_VALUE_HEADS
SAMPLES = 16
CHIPS = 8
D = 8192
BLOCKS = D // 128
WIDTH = 1024
ROWS = 40
SCALE = HEAD_SIZE ** (-0.5)
MASKED = -1e30
LOWEST = -1e29
F32 = jnp.float32
BF16 = jnp.bfloat16

LONG = pl.CostEstimate(flops=10**10, bytes_accessed=10**6, transcendentals=0)


def vmem(count):
    return [pl.BlockSpec(memory_space=pltpu.VMEM)] * count


def at_most(mebibytes):
    return pltpu.CompilerParams(vmem_limit_bytes=mebibytes * 2**20)


def smem(count):
    return [pl.BlockSpec(memory_space=pltpu.SMEM)] * count


def spread_kernel(query_ref, out_ref):
    rows = [query_ref[0:1, h * 128 : (h + 1) * 128].astype(F32) for h in range(HQ)]
    rows = jnp.concatenate(rows, axis=0).astype(BF16)
    for i in range(SAMPLES):
        out_ref[i] = rows


def attend_kernel(
    place_ref,
    prefix_len_ref,
    suffix_len_ref,
    query_ref,
    pkeys_ref,
    pvalues_ref,
    skeys_ref,
    svalues_ref,
    key_ref,
    value_ref,
    out_ref,
    queries,
):
    place = place_ref[0]
    queries[...] = query_ref[...].reshape(SAMPLES * HQ, 128).astype(F32)
    row = lax.broadcasted_iota(jnp.int32, (64, 128), 0)
    lane = lax.broadcasted_iota(jnp.int32, (64, 128), 1)
    sample = 2 * (row % 8) + row // 32
    prefix_seen = lane + place * 128 < prefix_len_ref[0]
    own_seen = (sample == place) & ((lane < suffix_len_ref[0]) | (lane == 64))
    first = row == 0
    mark = lane[:32] == row[:32] + 32 * (place % 4)
    ones = jnp.ones((256, 128), BF16)
    zeros = jnp.zeros((5, 128), F32)
    for k in range(KEY_VALUE_HEADS):
        head = slice(k * 128, (k + 1) * 128)
        new_key = jnp.where(first, key_ref[0:1, head].astype(F32), 0.0).astype(BF16)
        new_value = jnp.where(first, value_ref[0:1, head].astype(F32), 0.0).astype(BF16)
        keys = jnp.concatenate([pkeys_ref[:, head], skeys_ref[0, :, head], new_key], axis=0)
        values = jnp.concatenate([pvalues_ref[:, head], svalues_ref[0, :, head], new_value], axis=0)
        query = [
            queries[pl.ds(c * HQ + k * GROUP + g, 8, stride=2 * HQ), :]
            for c in range(2)
            for g in range(GROUP)
        ]
        query = jnp.concatenate(query, axis=0).astype(BF16)
        scores = lax.dot_general(
            query, keys, (((1,), (1,)), ((), ())), preferred_element_type=F32
        )
        s_pre = jnp.where(prefix_seen, scores[:, :128] * SCALE, MASKED)
        s_own = jnp.where(own_seen, scores[:, 128:] * SCALE, MASKED)
        top = jnp.max(jnp.maximum(s_pre, s_own), axis=-1, keepdims=True)
        top = jnp.maximum(top, LOWEST).astype(BF16).astype(F32)
        weights = jnp.concatenate([jnp.exp(s_pre - top), jnp.exp(s_own - top)], axis=1)
        summed = jnp.dot(
            weights.astype(BF16),
            jnp.concatenate([values, ones], axis=1),
            preferred_element_type=F32,
        )
        total = summed[:, 128:]
        total_high = total.astype(BF16).astype(F32)
        total_low = total - total_high
        for c in range(2):
            part = slice(32 * c, 32 * c + 32)
            out_ref[2 * k + c, 0:32, :] = summed[part, :128].astype(BF16)
            stats = [
                jnp.sum(jnp.where(mark, v[part], 0.0), axis=0, keepdims=True)
                for v in (top, total_high, total_low)
            ]
            out_ref[2 * k + c, 32:ROWS, :] = jnp.concatenate(stats + [zeros], axis=0).astype(BF16)


def project_kernel(place_ref, got_ref, own_ref, other_hbm, out_ref, rows, other_ref, arrived):
    copies = [
        pltpu.make_async_copy(
            other_hbm.at[:, n : n + WIDTH], other_ref.at[:, n : n + WIDTH], arrived.at[n // WIDTH]
        )
        for n in range(0, D, WIDTH)
    ]
    for copy in copies:
        copy.start()
    stats = got_ref[:, 32:ROWS, :].astype(F32)
    quads = [
        stats[4 * q] + stats[4 * q + 1] + stats[4 * q + 2] + stats[4 * q + 3] for q in range(4)
    ]
    tops = [s[0:1] for s in quads]
    totals = [s[1:2] + s[2:3] for s in quads]
    top = jnp.maximum(jnp.maximum(tops[0], tops[1]), jnp.maximum(tops[2], tops[3]))
    top = jnp.maximum(top, pltpu.roll(top, 64, 1))
    top = jnp.maximum(top, pltpu.roll(top, 32, 1))
    factors = [jnp.exp(t - top) for t in tops]
    total = sum(f * t for f, t in zip(factors, totals))
    total = total + pltpu.roll(total, 64, 1)
    total = total + pltpu.roll(total, 32, 1)
    row = lax.broadcasted_iota(jnp.int32, (32, 128), 0)
    lane = lax.broadcasted_iota(jnp.int32, (32, 128), 1)
    diagonal = lane % 32 == row
    mix = jnp.concatenate([jnp.where(diagonal, f / total, 0.0) for f in factors], axis=1)
    high = mix.astype(BF16)
    low = (mix - high.astype(F32)).astype(BF16)
    sums = got_ref[:, 0:32, :].reshape(SAMPLES * 32, 128)
    both = jnp.dot(jnp.concatenate([high, low], axis=0), sums, preferred_element_type=F32)
    attn = both[:32] + both[32:]
    attn = jnp.concatenate([attn[8 * g : 8 * g + 8] for g in range(GROUP)], axis=1)
    north = place_ref[0] % 2 == 1
    mine = jnp.where(north, attn[:, 256:], attn[:, :256]).astype(BF16)
    others = jnp.where(north, attn[:, :256], attn[:, 256:]).astype(BF16)
    for n in range(0, D, WIDTH):
        cols = slice(n, n + WIDTH)
        piece = jnp.dot(mine, own_ref[:, cols], preferred_element_type=F32)
        copies[n // WIDTH].wait()
        piece += jnp.dot(others, other_ref[:, cols], preferred_element_type=F32)
        for i in range(WIDTH // 128):
            rows[pl.ds(n // 128 + i, 8, stride=BLOCKS), :] = piece[:, 128 * i : 128 * i + 128]
    out_ref[...] = rows[...].astype(BF16).reshape(CHIPS, BLOCKS, 128)


def stage_kernel(residual_ref, gain_ref, residual_rows_ref, gain_rows_ref):
    rows = [residual_ref[0:1, 128 * i : 128 * i + 128].astype(F32) for i in range(BLOCKS)]
    residual_rows_ref[...] = jnp.concatenate(rows, axis=0)
    gain_rows_ref[...] = gain_ref[...].astype(F32)


def finish_kernel(got_ref, residual_ref, gain_ref, hidden_ref, normed_ref):
    proj = got_ref[0].astype(F32)
    for i in range(1, CHIPS):
        proj += got_ref[i].astype(F32)
    stream = residual_ref[...] + proj
    scale = lax.rsqrt(jnp.sum(stream * stream) * (1.0 / D) + 1e-05)
    normed = stream * scale * gain_ref[...]
    for i in range(BLOCKS):
        cols = slice(128 * i, 128 * i + 128)
        hidden_ref[0:1, cols] = stream[i : i + 1].astype(BF16)
        normed_ref[0:1, cols] = normed[i : i + 1].astype(BF16)


def local(
    query_new,
    key_new,
    value_new,
    prefix_keys,
    prefix_values,
    sample_suffix_keys,
    sample_suffix_values,
    prefix_len,
    suffix_len,
    residual,
    out_weight,
    norm_gain,
):
    place = lax.axis_index("mp").astype(jnp.int32)[None]
    cores = [[2 * z + c for z in range(CHIPS)] for c in range(2)]
    other_weight = lax.ppermute(out_weight, "mp", [(i, i ^ 1) for i in range(SAMPLES)])
    spread = pl.pallas_call(
        spread_kernel,
        out_shape=jax.ShapeDtypeStruct((SAMPLES, HQ, 128), BF16),
        in_specs=vmem(1),
        out_specs=vmem(1)[0],
        compiler_params=at_most(2),
        cost_estimate=LONG,
    )(query_new)
    queries = lax.all_to_all(spread, "mp", 0, 0, tiled=True)
    residual_rows, gain_rows = pl.pallas_call(
        stage_kernel,
        out_shape=[jax.ShapeDtypeStruct((BLOCKS, 128), F32)] * 2,
        in_specs=vmem(2),
        out_specs=vmem(2),
        compiler_params=at_most(2),
        cost_estimate=LONG,
    )(residual, norm_gain.reshape(BLOCKS, 128))
    partial = pl.pallas_call(
        attend_kernel,
        out_shape=jax.ShapeDtypeStruct((SAMPLES, ROWS, 128), BF16),
        in_specs=smem(3) + vmem(7),
        out_specs=vmem(1)[0],
        scratch_shapes=[pltpu.VMEM((SAMPLES * HQ, 128), F32)],
        compiler_params=at_most(8),
        cost_estimate=LONG,
    )(
        place,
        prefix_len,
        suffix_len,
        queries,
        prefix_keys,
        prefix_values,
        sample_suffix_keys,
        sample_suffix_values,
        key_new,
        value_new,
    )
    partial = lax.all_to_all(partial, "mp", 0, 0, tiled=True)
    proj = pl.pallas_call(
        project_kernel,
        out_shape=jax.ShapeDtypeStruct((CHIPS, BLOCKS, 128), BF16),
        in_specs=smem(1) + vmem(2) + [pl.BlockSpec(memory_space=pl.ANY)],
        out_specs=vmem(1)[0],
        scratch_shapes=[
            pltpu.VMEM((8 * BLOCKS, 128), F32),
            pltpu.VMEM((256, D), BF16),
            pltpu.SemaphoreType.DMA((D // WIDTH,)),
        ],
        compiler_params=at_most(16),
        cost_estimate=LONG,
    )(place, partial, out_weight, other_weight)
    proj = lax.all_to_all(proj, "mp", 0, 0, tiled=True, axis_index_groups=cores)
    return tuple(
        pl.pallas_call(
            finish_kernel,
            out_shape=[jax.ShapeDtypeStruct((1, D), BF16)] * 2,
            in_specs=vmem(3),
            out_specs=vmem(2),
            compiler_params=at_most(4),
        )(proj, residual_rows, gain_rows)
    )


def solution(mesh):
    whole = P(("dp", "mp"), None)
    placed = (
        whole,
        whole,
        whole,
        whole,
        whole,
        P(("dp", "mp"), None, None),
        P(("dp", "mp"), None, None),
        P("dp"),
        P(("dp", "mp")),
        whole,
        P("mp", None),
        P(),
    )

    def step(*arrays):
        return local(*arrays)

    step = jax.shard_map(
        step, mesh=mesh, in_specs=placed, out_specs=(whole, whole), check_vma=False
    )
    return step
```

```python
import jax
import jax.numpy as jnp
from jax import lax
from jax.experimental import pallas as pl
from jax.experimental.pallas import tpu as pltpu
from jax.sharding import PartitionSpec as P


HEAD_SIZE = 128
KEY_VALUE_HEADS = 8
HQ = 32
GROUP = HQ // KEY_VALUE_HEADS
SAMPLES = 16
CHIPS = 8
D = 8192
BLOCKS = D // 128
WIDTH = 1024
ROWS = 40
SCALE = HEAD_SIZE ** (-0.5)
MASKED = -1e30
LOWEST = -1e29
F32 = jnp.float32
BF16 = jnp.bfloat16

LONG = pl.CostEstimate(flops=10**10, bytes_accessed=10**6, transcendentals=0)


def vmem(count):
    return [pl.BlockSpec(memory_space=pltpu.VMEM)] * count


def hbm(count):
    return [pl.BlockSpec(memory_space=pltpu.HBM)] * count


def at_most(mebibytes):
    return pltpu.CompilerParams(vmem_limit_bytes=mebibytes * 2**20)


def smem(count):
    return [pl.BlockSpec(memory_space=pltpu.SMEM)] * count


def spread_kernel(query_ref, out_ref):
    rows = [query_ref[0:1, h * 128 : (h + 1) * 128].astype(F32) for h in range(HQ)]
    rows = jnp.concatenate(rows, axis=0).astype(BF16)
    for i in range(CHIPS):
        out_ref[i] = rows


def stage_kernel(
    place_ref,
    prefix_len_hbm,
    suffix_len_hbm,
    pkeys_ref,
    pvalues_ref,
    skeys_ref,
    svalues_ref,
    key_ref,
    value_ref,
    residual_ref,
    gain_ref,
    prefix_ref,
    own_ref,
    bias_ref,
    residual_rows_ref,
    gain_rows_ref,
    lengths,
    arrived,
):
    copies = [
        pltpu.make_async_copy(source, lengths.at[i], arrived.at[i])
        for i, source in enumerate((prefix_len_hbm, suffix_len_hbm))
    ]
    for copy in copies:
        copy.start()
    prefix_ref[:128] = pkeys_ref[...]
    prefix_ref[128:] = pvalues_ref[...]
    first = lax.broadcasted_iota(jnp.int32, (64, 1024), 0) == 0
    own_ref[0:64] = skeys_ref[0]
    own_ref[64:128] = jnp.where(first, key_ref[...].astype(F32), 0.0).astype(BF16)
    own_ref[128:192] = svalues_ref[0]
    own_ref[192:256] = jnp.where(first, value_ref[...].astype(F32), 0.0).astype(BF16)
    rows = [residual_ref[0:1, 128 * i : 128 * i + 128].astype(F32) for i in range(BLOCKS)]
    residual_rows_ref[...] = jnp.concatenate(rows, axis=0)
    gain_rows_ref[...] = gain_ref[...].astype(F32)
    for copy in copies:
        copy.wait()
    place = place_ref[0]
    row = lax.broadcasted_iota(jnp.int32, (32, 128), 0)
    lane = lax.broadcasted_iota(jnp.int32, (32, 128), 1)
    prefix_len = lengths[0, 0]
    other_place = place + 1 - 2 * (place % 2)
    own = (row % 8 == place // 2) & ((lane < lengths[1, 0]) | (lane == 64))
    seen = (lane + place * 128 < prefix_len, lane + other_place * 128 < prefix_len, own)
    for i, mask in enumerate(seen):
        bias_ref[i] = jnp.where(mask, 0.0, MASKED)


def attend_kernel(
    place_ref,
    weight_hbm,
    query_ref,
    prefix_ref,
    other_ref,
    own_ref,
    bias_ref,
    out_ref,
    weight_ref,
    queries,
    arrived,
):
    copy = pltpu.make_async_copy(weight_hbm, weight_ref, arrived)
    copy.start()
    queries[...] = query_ref[...].reshape(CHIPS * HQ, 128).astype(F32)
    row = lax.broadcasted_iota(jnp.int32, (32, 128), 0)
    lane = lax.broadcasted_iota(jnp.int32, (32, 128), 1)
    mark = lane == row + 32 * (place_ref[0] // 2 % 4)
    ones = jnp.ones((384, 128), BF16)
    zeros = jnp.zeros((5, 128), F32)
    for k in range(KEY_VALUE_HEADS):
        head = slice(k * 128, (k + 1) * 128)
        parts = (prefix_ref, other_ref, own_ref)
        keys = jnp.concatenate([part[:128, head] for part in parts], axis=0)
        values = jnp.concatenate([part[128:, head] for part in parts], axis=0)
        query = [queries[pl.ds(k * GROUP + g, 8, stride=HQ), :] for g in range(GROUP)]
        query = jnp.concatenate(query, axis=0).astype(BF16)
        scores = lax.dot_general(
            query, keys, (((1,), (1,)), ((), ())), preferred_element_type=F32
        )
        scores = [scores[:, 128 * i : 128 * i + 128] * SCALE + bias_ref[i] for i in range(3)]
        top = jnp.maximum(jnp.maximum(scores[0], scores[1]), scores[2])
        top = jnp.max(top, axis=-1, keepdims=True)
        top = jnp.maximum(top, LOWEST).astype(BF16).astype(F32)
        weights = jnp.concatenate([jnp.exp(s - top) for s in scores], axis=1)
        summed = jnp.dot(
            weights.astype(BF16),
            jnp.concatenate([values, ones], axis=1),
            preferred_element_type=F32,
        )
        total = summed[:, 128:]
        total_high = total.astype(BF16).astype(F32)
        total_low = total - total_high
        out_ref[k, 0:32, :] = summed[:, :128].astype(BF16)
        stats = [
            jnp.sum(jnp.where(mark, v, 0.0), axis=0, keepdims=True)
            for v in (top, total_high, total_low)
        ]
        out_ref[k, 32:ROWS, :] = jnp.concatenate(stats + [zeros], axis=0).astype(BF16)
    copy.wait()


def project_kernel(place_ref, got_ref, own_ref, other_hbm, out_ref, rows, other_ref, arrived):
    copies = [
        pltpu.make_async_copy(
            other_hbm.at[:, n : n + WIDTH], other_ref.at[:, n : n + WIDTH], arrived.at[n // WIDTH]
        )
        for n in range(0, D, WIDTH)
    ]
    for copy in copies:
        copy.start()
    stats = got_ref[:, 32:ROWS, :].astype(F32)
    quads = [
        stats[4 * q] + stats[4 * q + 1] + stats[4 * q + 2] + stats[4 * q + 3] for q in range(2)
    ]
    tops = [s[0:1] for s in quads]
    totals = [s[1:2] + s[2:3] for s in quads]
    top = jnp.maximum(tops[0], tops[1])
    top = jnp.maximum(top, pltpu.roll(top, 64, 1))
    top = jnp.maximum(top, pltpu.roll(top, 32, 1))
    factors = [jnp.exp(t - top) for t in tops]
    total = sum(f * t for f, t in zip(factors, totals))
    total = total + pltpu.roll(total, 64, 1)
    total = total + pltpu.roll(total, 32, 1)
    row = lax.broadcasted_iota(jnp.int32, (32, 128), 0)
    lane = lax.broadcasted_iota(jnp.int32, (32, 128), 1)
    diagonal = lane % 32 == row
    mix = jnp.concatenate([jnp.where(diagonal, f / total, 0.0) for f in factors], axis=1)
    high = mix.astype(BF16)
    low = (mix - high.astype(F32)).astype(BF16)
    sums = got_ref[:, 0:32, :].reshape(CHIPS * 32, 128)
    both = jnp.dot(jnp.concatenate([high, low], axis=0), sums, preferred_element_type=F32)
    attn = both[:32] + both[32:]
    attn = jnp.concatenate([attn[8 * g : 8 * g + 8] for g in range(GROUP)], axis=1)
    north = place_ref[0] % 2 == 1
    mine = jnp.where(north, attn[:, 256:], attn[:, :256]).astype(BF16)
    others = jnp.where(north, attn[:, :256], attn[:, 256:]).astype(BF16)
    for n in range(0, D, WIDTH):
        cols = slice(n, n + WIDTH)
        piece = jnp.dot(mine, own_ref[:, cols], preferred_element_type=F32)
        copies[n // WIDTH].wait()
        piece += jnp.dot(others, other_ref[:, cols], preferred_element_type=F32)
        for i in range(WIDTH // 128):
            rows[pl.ds(n // 128 + i, 8, stride=BLOCKS), :] = piece[:, 128 * i : 128 * i + 128]
    out_ref[...] = rows[...].astype(BF16).reshape(CHIPS, BLOCKS, 128)


def finish_kernel(got_ref, residual_ref, gain_ref, hidden_ref, normed_ref):
    proj = got_ref[0].astype(F32)
    for i in range(1, CHIPS):
        proj += got_ref[i].astype(F32)
    stream = residual_ref[...] + proj
    scale = lax.rsqrt(jnp.sum(stream * stream) * (1.0 / D) + 1e-05)
    normed = stream * scale * gain_ref[...]
    for i in range(BLOCKS):
        cols = slice(128 * i, 128 * i + 128)
        hidden_ref[0:1, cols] = stream[i : i + 1].astype(BF16)
        normed_ref[0:1, cols] = normed[i : i + 1].astype(BF16)


def local(
    query_new,
    key_new,
    value_new,
    prefix_keys,
    prefix_values,
    sample_suffix_keys,
    sample_suffix_values,
    prefix_len,
    suffix_len,
    residual,
    out_weight,
    norm_gain,
):
    place = lax.axis_index("mp").astype(jnp.int32)[None]
    cores = [[2 * z + c for z in range(CHIPS)] for c in range(2)]
    swapped = [(i, i ^ 1) for i in range(SAMPLES)]
    spread = pl.pallas_call(
        spread_kernel,
        out_shape=jax.ShapeDtypeStruct((CHIPS, HQ, 128), BF16),
        in_specs=vmem(1),
        out_specs=vmem(1)[0],
        compiler_params=at_most(2),
        cost_estimate=LONG,
    )(query_new)
    queries = lax.all_to_all(spread, "mp", 0, 0, tiled=True, axis_index_groups=cores)
    prefix, own, bias, residual_rows, gain_rows = pl.pallas_call(
        stage_kernel,
        out_shape=[
            jax.ShapeDtypeStruct((256, 1024), BF16),
            jax.ShapeDtypeStruct((256, 1024), BF16),
            jax.ShapeDtypeStruct((3, 32, 128), F32),
            jax.ShapeDtypeStruct((BLOCKS, 128), F32),
            jax.ShapeDtypeStruct((BLOCKS, 128), F32),
        ],
        in_specs=smem(1) + hbm(2) + vmem(8),
        out_specs=vmem(5),
        scratch_shapes=[pltpu.SMEM((2, 1), jnp.int32), pltpu.SemaphoreType.DMA((2,))],
        compiler_params=at_most(4),
        cost_estimate=LONG,
    )(
        place,
        prefix_len,
        suffix_len,
        prefix_keys,
        prefix_values,
        sample_suffix_keys,
        sample_suffix_values,
        key_new,
        value_new,
        residual,
        norm_gain.reshape(BLOCKS, 128),
    )
    other_prefix = lax.ppermute(prefix, "mp", swapped)
    other_weight = lax.ppermute(out_weight, "mp", swapped)
    partial, weight = pl.pallas_call(
        attend_kernel,
        out_shape=[
            jax.ShapeDtypeStruct((CHIPS, ROWS, 128), BF16),
            jax.ShapeDtypeStruct((256, D), BF16),
        ],
        in_specs=smem(1) + hbm(1) + vmem(5),
        out_specs=vmem(2),
        scratch_shapes=[pltpu.VMEM((CHIPS * HQ, 128), F32), pltpu.SemaphoreType.DMA],
        compiler_params=at_most(12),
        cost_estimate=LONG,
    )(place, out_weight, queries, prefix, other_prefix, own, bias)
    partial = lax.all_to_all(partial, "mp", 0, 0, tiled=True, axis_index_groups=cores)
    proj = pl.pallas_call(
        project_kernel,
        out_shape=jax.ShapeDtypeStruct((CHIPS, BLOCKS, 128), BF16),
        in_specs=smem(1) + vmem(2) + hbm(1),
        out_specs=vmem(1)[0],
        scratch_shapes=[
            pltpu.VMEM((8 * BLOCKS, 128), F32),
            pltpu.VMEM((256, D), BF16),
            pltpu.SemaphoreType.DMA((D // WIDTH,)),
        ],
        compiler_params=at_most(16),
        cost_estimate=LONG,
    )(place, partial, weight, other_weight)
    proj = lax.all_to_all(proj, "mp", 0, 0, tiled=True, axis_index_groups=cores)
    return tuple(
        pl.pallas_call(
            finish_kernel,
            out_shape=[jax.ShapeDtypeStruct((1, D), BF16)] * 2,
            in_specs=vmem(3),
            out_specs=vmem(2),
            compiler_params=at_most(4),
        )(proj, residual_rows, gain_rows)
    )


def solution(mesh):
    whole = P(("dp", "mp"), None)
    placed = (
        whole,
        whole,
        whole,
        whole,
        whole,
        P(("dp", "mp"), None, None),
        P(("dp", "mp"), None, None),
        P("dp"),
        P(("dp", "mp")),
        whole,
        P("mp", None),
        P(),
    )

    def step(*arrays):
        return local(*arrays)

    step = jax.shard_map(
        step, mesh=mesh, in_specs=placed, out_specs=(whole, whole), check_vma=False
    )
    return step
```

```python
import jax
import jax.numpy as jnp
from jax import lax
from jax.experimental import pallas as pl
from jax.experimental.pallas import tpu as pltpu
from jax.sharding import PartitionSpec as P


HEAD_SIZE = 128
KEY_VALUE_HEADS = 8
HQ = 32
GROUP = HQ // KEY_VALUE_HEADS
SAMPLES = 16
CHIPS = 8
D = 8192
BLOCKS = D // 128
WIDTH = 1024
ROWS = 40
SCALE = HEAD_SIZE ** (-0.5)
MASKED = -1e30
LOWEST = -1e29
F32 = jnp.float32
BF16 = jnp.bfloat16

LONG = pl.CostEstimate(flops=10**10, bytes_accessed=10**6, transcendentals=0)


def vmem(count):
    return [pl.BlockSpec(memory_space=pltpu.VMEM)] * count


def hbm(count):
    return [pl.BlockSpec(memory_space=pltpu.HBM)] * count


def at_most(mebibytes):
    return pltpu.CompilerParams(vmem_limit_bytes=mebibytes * 2**20)


def smem(count):
    return [pl.BlockSpec(memory_space=pltpu.SMEM)] * count


def spread_kernel(query_ref, out_ref):
    rows = [query_ref[0:1, h * 128 : (h + 1) * 128].astype(F32) for h in range(HQ)]
    rows = jnp.concatenate(rows, axis=0).astype(BF16)
    for i in range(SAMPLES):
        out_ref[i] = rows


def stage_kernel(
    place_ref,
    prefix_len_ref,
    suffix_len_ref,
    skeys_ref,
    svalues_ref,
    key_ref,
    value_ref,
    residual_ref,
    gain_ref,
    own_ref,
    bias_ref,
    residual_rows_ref,
    gain_rows_ref,
):
    first = lax.broadcasted_iota(jnp.int32, (64, 1024), 0) == 0
    own_ref[0:64] = skeys_ref[0]
    own_ref[64:128] = jnp.where(first, key_ref[...].astype(F32), 0.0).astype(BF16)
    own_ref[128:192] = svalues_ref[0]
    own_ref[192:256] = jnp.where(first, value_ref[...].astype(F32), 0.0).astype(BF16)
    rows = [residual_ref[0:1, 128 * i : 128 * i + 128].astype(F32) for i in range(BLOCKS)]
    residual_rows_ref[...] = jnp.concatenate(rows, axis=0)
    gain_rows_ref[...] = gain_ref[...].astype(F32)
    place = place_ref[0]
    row = lax.broadcasted_iota(jnp.int32, (64, 128), 0)
    lane = lax.broadcasted_iota(jnp.int32, (64, 128), 1)
    sample = 2 * (row % 8) + row // 32
    own = (sample == place) & ((lane < suffix_len_ref[0]) | (lane == 64))
    bias_ref[0] = jnp.where(lane + place * 128 < prefix_len_ref[0], 0.0, MASKED)
    bias_ref[1] = jnp.where(own, 0.0, MASKED)


def attend_kernel(
    place_ref, query_ref, pkeys_ref, pvalues_ref, own_ref, bias_ref, out_ref, queries
):
    queries[...] = query_ref[...].reshape(SAMPLES * HQ, 128).astype(F32)
    row = lax.broadcasted_iota(jnp.int32, (32, 128), 0)
    lane = lax.broadcasted_iota(jnp.int32, (32, 128), 1)
    mark = lane == row + 32 * (place_ref[0] % 4)
    ones = jnp.ones((256, 128), BF16)
    zeros = jnp.zeros((5, 128), F32)
    for k in range(KEY_VALUE_HEADS):
        head = slice(k * 128, (k + 1) * 128)
        keys = jnp.concatenate([pkeys_ref[:, head], own_ref[:128, head]], axis=0)
        values = jnp.concatenate([pvalues_ref[:, head], own_ref[128:, head]], axis=0)
        query = [
            queries[pl.ds(c * HQ + k * GROUP + g, 8, stride=2 * HQ), :]
            for c in range(2)
            for g in range(GROUP)
        ]
        query = jnp.concatenate(query, axis=0).astype(BF16)
        scores = lax.dot_general(
            query, keys, (((1,), (1,)), ((), ())), preferred_element_type=F32
        )
        s_pre = scores[:, :128] * SCALE + bias_ref[0]
        s_own = scores[:, 128:] * SCALE + bias_ref[1]
        top = jnp.max(jnp.maximum(s_pre, s_own), axis=-1, keepdims=True)
        top = jnp.maximum(top, LOWEST).astype(BF16).astype(F32)
        weights = jnp.concatenate([jnp.exp(s_pre - top), jnp.exp(s_own - top)], axis=1)
        summed = jnp.dot(
            weights.astype(BF16),
            jnp.concatenate([values, ones], axis=1),
            preferred_element_type=F32,
        )
        total = summed[:, 128:]
        total_high = total.astype(BF16).astype(F32)
        total_low = total - total_high
        for c in range(2):
            part = slice(32 * c, 32 * c + 32)
            out_ref[2 * k + c, 0:32, :] = summed[part, :128].astype(BF16)
            stats = [
                jnp.sum(jnp.where(mark, v[part], 0.0), axis=0, keepdims=True)
                for v in (top, total_high, total_low)
            ]
            out_ref[2 * k + c, 32:ROWS, :] = jnp.concatenate(stats + [zeros], axis=0).astype(BF16)


def project_kernel(place_ref, got_ref, own_ref, other_hbm, out_ref, halves, rows, other_ref, arrived):
    copies = [
        pltpu.make_async_copy(
            other_hbm.at[:, n : n + WIDTH], other_ref.at[:, n : n + WIDTH], arrived.at[n // WIDTH]
        )
        for n in range(0, D, WIDTH)
    ]
    for copy in copies:
        copy.start()
    stats = got_ref[:, 32:ROWS, :].astype(F32)
    quads = [
        stats[4 * q] + stats[4 * q + 1] + stats[4 * q + 2] + stats[4 * q + 3] for q in range(4)
    ]
    tops = [s[0:1] for s in quads]
    totals = [s[1:2] + s[2:3] for s in quads]
    top = jnp.maximum(jnp.maximum(tops[0], tops[1]), jnp.maximum(tops[2], tops[3]))
    top = jnp.maximum(top, pltpu.roll(top, 64, 1))
    top = jnp.maximum(top, pltpu.roll(top, 32, 1))
    factors = [jnp.exp(t - top) for t in tops]
    total = sum(f * t for f, t in zip(factors, totals))
    total = total + pltpu.roll(total, 64, 1)
    total = total + pltpu.roll(total, 32, 1)
    row = lax.broadcasted_iota(jnp.int32, (32, 128), 0)
    lane = lax.broadcasted_iota(jnp.int32, (32, 128), 1)
    diagonal = lane % 32 == row
    mix = jnp.concatenate([jnp.where(diagonal, f / total, 0.0) for f in factors], axis=1)
    high = mix.astype(BF16)
    low = (mix - high.astype(F32)).astype(BF16)
    sums = got_ref[:, 0:32, :].reshape(SAMPLES * 32, 128)
    both = jnp.dot(jnp.concatenate([high, low], axis=0), sums, preferred_element_type=F32)
    attn = both[:32] + both[32:]
    attn = jnp.concatenate([attn[8 * g : 8 * g + 8] for g in range(GROUP)], axis=1)
    north = place_ref[0] % 2 == 1
    mine = jnp.where(north, attn[:, 256:], attn[:, :256]).astype(BF16)
    others = jnp.where(north, attn[:, :256], attn[:, 256:]).astype(BF16)
    for n in range(0, D, WIDTH):
        cols = slice(n, n + WIDTH)
        halves[:, cols] = jnp.dot(mine, own_ref[:, cols], preferred_element_type=F32)
    for n, copy in zip(range(0, D, WIDTH), copies):
        cols = slice(n, n + WIDTH)
        copy.wait()
        piece = halves[:, cols] + jnp.dot(others, other_ref[:, cols], preferred_element_type=F32)
        for i in range(WIDTH // 128):
            rows[pl.ds(n // 128 + i, 8, stride=BLOCKS), :] = piece[:, 128 * i : 128 * i + 128]
    out_ref[...] = rows[...].astype(BF16).reshape(CHIPS, BLOCKS, 128)


def finish_kernel(got_ref, residual_ref, gain_ref, hidden_ref, normed_ref):
    proj = got_ref[0].astype(F32)
    for i in range(1, CHIPS):
        proj += got_ref[i].astype(F32)
    stream = residual_ref[...] + proj
    scale = lax.rsqrt(jnp.sum(stream * stream) * (1.0 / D) + 1e-05)
    normed = stream * scale * gain_ref[...]
    for i in range(BLOCKS):
        cols = slice(128 * i, 128 * i + 128)
        hidden_ref[0:1, cols] = stream[i : i + 1].astype(BF16)
        normed_ref[0:1, cols] = normed[i : i + 1].astype(BF16)


def local(
    query_new,
    key_new,
    value_new,
    prefix_keys,
    prefix_values,
    sample_suffix_keys,
    sample_suffix_values,
    prefix_len,
    suffix_len,
    residual,
    out_weight,
    norm_gain,
):
    place = lax.axis_index("mp").astype(jnp.int32)[None]
    cores = [[2 * z + c for z in range(CHIPS)] for c in range(2)]
    spread = pl.pallas_call(
        spread_kernel,
        out_shape=jax.ShapeDtypeStruct((SAMPLES, HQ, 128), BF16),
        in_specs=vmem(1),
        out_specs=vmem(1)[0],
        compiler_params=at_most(2),
        cost_estimate=LONG,
    )(query_new)
    queries = lax.all_to_all(spread, "mp", 0, 0, tiled=True)
    own, bias, residual_rows, gain_rows = pl.pallas_call(
        stage_kernel,
        out_shape=[
            jax.ShapeDtypeStruct((256, 1024), BF16),
            jax.ShapeDtypeStruct((2, 64, 128), F32),
            jax.ShapeDtypeStruct((BLOCKS, 128), F32),
            jax.ShapeDtypeStruct((BLOCKS, 128), F32),
        ],
        in_specs=smem(3) + vmem(6),
        out_specs=vmem(4),
        compiler_params=at_most(4),
        cost_estimate=LONG,
    )(
        place,
        prefix_len,
        suffix_len,
        sample_suffix_keys,
        sample_suffix_values,
        key_new,
        value_new,
        residual,
        norm_gain.reshape(BLOCKS, 128),
    )
    other_weight = lax.ppermute(out_weight, "mp", [(i, i ^ 1) for i in range(SAMPLES)])
    partial = pl.pallas_call(
        attend_kernel,
        out_shape=jax.ShapeDtypeStruct((SAMPLES, ROWS, 128), BF16),
        in_specs=smem(1) + vmem(5),
        out_specs=vmem(1)[0],
        scratch_shapes=[pltpu.VMEM((SAMPLES * HQ, 128), F32)],
        compiler_params=at_most(8),
        cost_estimate=LONG,
    )(place, queries, prefix_keys, prefix_values, own, bias)
    partial = lax.all_to_all(partial, "mp", 0, 0, tiled=True)
    proj = pl.pallas_call(
        project_kernel,
        out_shape=jax.ShapeDtypeStruct((CHIPS, BLOCKS, 128), BF16),
        in_specs=smem(1) + vmem(2) + hbm(1),
        out_specs=vmem(1)[0],
        scratch_shapes=[
            pltpu.VMEM((8, D), F32),
            pltpu.VMEM((8 * BLOCKS, 128), F32),
            pltpu.VMEM((256, D), BF16),
            pltpu.SemaphoreType.DMA((D // WIDTH,)),
        ],
        compiler_params=at_most(16),
        cost_estimate=LONG,
    )(place, partial, out_weight, other_weight)
    proj = lax.all_to_all(proj, "mp", 0, 0, tiled=True, axis_index_groups=cores)
    return tuple(
        pl.pallas_call(
            finish_kernel,
            out_shape=[jax.ShapeDtypeStruct((1, D), BF16)] * 2,
            in_specs=vmem(3),
            out_specs=vmem(2),
            compiler_params=at_most(4),
        )(proj, residual_rows, gain_rows)
    )


def solution(mesh):
    whole = P(("dp", "mp"), None)
    placed = (
        whole,
        whole,
        whole,
        whole,
        whole,
        P(("dp", "mp"), None, None),
        P(("dp", "mp"), None, None),
        P("dp"),
        P(("dp", "mp")),
        whole,
        P("mp", None),
        P(),
    )

    def step(*arrays):
        return local(*arrays)

    step = jax.shard_map(
        step, mesh=mesh, in_specs=placed, out_specs=(whole, whole), check_vma=False
    )
    return step
```

```python
import jax
import jax.numpy as jnp
from jax import lax
from jax.experimental import pallas as pl
from jax.experimental.pallas import tpu as pltpu
from jax.sharding import PartitionSpec as P


HEAD_SIZE = 128
KEY_VALUE_HEADS = 8
HQ = 32
GROUP = HQ // KEY_VALUE_HEADS
SAMPLES = 16
CHIPS = 8
D = 8192
BLOCKS = D // 128
WIDTH = 2048
ROWS = 18
SCALE = HEAD_SIZE ** (-0.5)
MASKED = -1e30
LOWEST = -1e29
F32 = jnp.float32
BF16 = jnp.bfloat16

LONG = pl.CostEstimate(flops=10**10, bytes_accessed=10**6, transcendentals=0)


def vmem(count):
    return [pl.BlockSpec(memory_space=pltpu.VMEM)] * count


def hbm(count):
    return [pl.BlockSpec(memory_space=pltpu.HBM)] * count


def at_most(mebibytes):
    return pltpu.CompilerParams(vmem_limit_bytes=mebibytes * 2**20)


def smem(count):
    return [pl.BlockSpec(memory_space=pltpu.SMEM)] * count


def spread_kernel(query_ref, out_ref):
    rows = [query_ref[0:1, h * 128 : (h + 1) * 128].astype(F32) for h in range(HQ)]
    rows = jnp.concatenate(rows, axis=0).astype(BF16)
    for i in range(SAMPLES):
        out_ref[i] = rows


def stage_kernel(
    place_ref,
    prefix_len_ref,
    suffix_len_ref,
    skeys_ref,
    svalues_ref,
    key_ref,
    value_ref,
    residual_ref,
    gain_ref,
    own_ref,
    bias_ref,
    residual_rows_ref,
    gain_rows_ref,
):
    first = lax.broadcasted_iota(jnp.int32, (64, 1024), 0) == 0
    own_ref[0:64] = skeys_ref[0]
    own_ref[64:128] = jnp.where(first, key_ref[...].astype(F32), 0.0).astype(BF16)
    own_ref[128:192] = svalues_ref[0]
    own_ref[192:256] = jnp.where(first, value_ref[...].astype(F32), 0.0).astype(BF16)
    rows = [residual_ref[0:1, 128 * i : 128 * i + 128].astype(F32) for i in range(BLOCKS)]
    residual_rows_ref[...] = jnp.concatenate(rows, axis=0)
    gain_rows_ref[...] = gain_ref[...].astype(F32)
    place = place_ref[0]
    row = lax.broadcasted_iota(jnp.int32, (64, 128), 0)
    lane = lax.broadcasted_iota(jnp.int32, (64, 128), 1)
    sample = 2 * (row % 8) + row // 32
    own = (sample == place) & ((lane < suffix_len_ref[0]) | (lane == 64))
    bias_ref[0] = jnp.where(lane + place * 128 < prefix_len_ref[0], 0.0, MASKED)
    bias_ref[1] = jnp.where(own, 0.0, MASKED)


def attend_kernel(
    place_ref, query_ref, pkeys_ref, pvalues_ref, own_ref, bias_ref, out_ref, queries
):
    queries[...] = query_ref[...].reshape(SAMPLES * HQ, 128).astype(F32)
    row = lax.broadcasted_iota(jnp.int32, (32, 128), 0)
    lane = lax.broadcasted_iota(jnp.int32, (32, 128), 1)
    mark = lane == row + 32 * (place_ref[0] % 4)
    ones = jnp.ones((256, 128), BF16)
    zeros = jnp.zeros((1, 128), F32)
    for k in range(KEY_VALUE_HEADS):
        head = slice(k * 128, (k + 1) * 128)
        keys = jnp.concatenate([pkeys_ref[:, head], own_ref[:128, head]], axis=0)
        values = jnp.concatenate([pvalues_ref[:, head], own_ref[128:, head]], axis=0)
        query = [
            queries[pl.ds(c * HQ + k * GROUP + g, 8, stride=2 * HQ), :]
            for c in range(2)
            for g in range(GROUP)
        ]
        query = jnp.concatenate(query, axis=0).astype(BF16)
        scores = lax.dot_general(
            query, keys, (((1,), (1,)), ((), ())), preferred_element_type=F32
        )
        s_pre = scores[:, :128] * SCALE + bias_ref[0]
        s_own = scores[:, 128:] * SCALE + bias_ref[1]
        top = jnp.max(jnp.maximum(s_pre, s_own), axis=-1, keepdims=True)
        top = jnp.maximum(top, LOWEST).astype(BF16).astype(F32)
        weights = jnp.concatenate([jnp.exp(s_pre - top), jnp.exp(s_own - top)], axis=1)
        summed = jnp.dot(
            weights.astype(BF16),
            jnp.concatenate([values, ones], axis=1),
            preferred_element_type=F32,
        )
        total = summed[:, 128:]
        total_high = total.astype(BF16).astype(F32)
        total_low = total - total_high
        for c in range(2):
            part = slice(32 * c, 32 * c + 32)
            out_ref[2 * k + c, 0:16] = summed[part, :128].astype(BF16).reshape(16, 2, 128)
            stats = [
                jnp.sum(jnp.where(mark, v[part], 0.0), axis=0, keepdims=True)
                for v in (top, total_high, total_low)
            ]
            out_ref[2 * k + c, 16:ROWS] = jnp.concatenate(stats + [zeros], axis=0).astype(BF16).reshape(2, 2, 128)


def project_kernel(place_ref, got_ref, own_ref, other_hbm, out_ref, halves, rows, other_ref, arrived):
    copies = [
        pltpu.make_async_copy(
            other_hbm.at[:, n : n + WIDTH], other_ref.at[:, n : n + WIDTH], arrived.at[n // WIDTH]
        )
        for n in range(0, D, WIDTH)
    ]
    for copy in copies:
        copy.start()
    stats = got_ref[:, 16:ROWS].reshape(SAMPLES, 4, 128).astype(F32)
    quads = [
        stats[4 * q] + stats[4 * q + 1] + stats[4 * q + 2] + stats[4 * q + 3] for q in range(4)
    ]
    tops = [s[0:1] for s in quads]
    totals = [s[1:2] + s[2:3] for s in quads]
    top = jnp.maximum(jnp.maximum(tops[0], tops[1]), jnp.maximum(tops[2], tops[3]))
    top = jnp.maximum(top, pltpu.roll(top, 64, 1))
    top = jnp.maximum(top, pltpu.roll(top, 32, 1))
    factors = [jnp.exp(t - top) for t in tops]
    total = sum(f * t for f, t in zip(factors, totals))
    total = total + pltpu.roll(total, 64, 1)
    total = total + pltpu.roll(total, 32, 1)
    row = lax.broadcasted_iota(jnp.int32, (32, 128), 0)
    lane = lax.broadcasted_iota(jnp.int32, (32, 128), 1)
    diagonal = lane % 32 == row
    mix = jnp.concatenate([jnp.where(diagonal, f / total, 0.0) for f in factors], axis=1)
    high = mix.astype(BF16)
    low = (mix - high.astype(F32)).astype(BF16)
    sums = got_ref[:, 0:16].reshape(SAMPLES * 32, 128)
    both = jnp.dot(jnp.concatenate([high, low], axis=0), sums, preferred_element_type=F32)
    attn = both[:32] + both[32:]
    attn = jnp.concatenate([attn[8 * g : 8 * g + 8] for g in range(GROUP)], axis=1)
    north = place_ref[0] % 2 == 1
    mine = jnp.where(north, attn[:, 256:], attn[:, :256]).astype(BF16)
    others = jnp.where(north, attn[:, :256], attn[:, 256:]).astype(BF16)
    for n in range(0, D, WIDTH):
        cols = slice(n, n + WIDTH)
        halves[:, cols] = jnp.dot(mine, own_ref[:, cols], preferred_element_type=F32)
    for n, copy in zip(range(0, D, WIDTH), copies):
        cols = slice(n, n + WIDTH)
        copy.wait()
        piece = halves[:, cols] + jnp.dot(others, other_ref[:, cols], preferred_element_type=F32)
        for i in range(WIDTH // 128):
            rows[pl.ds(n // 128 + i, 8, stride=BLOCKS), :] = piece[:, 128 * i : 128 * i + 128]
    out_ref[...] = rows[...].astype(BF16).reshape(CHIPS, BLOCKS, 128)


def finish_kernel(got_ref, residual_ref, gain_ref, hidden_ref, normed_ref):
    proj = got_ref[0].astype(F32)
    for i in range(1, CHIPS):
        proj += got_ref[i].astype(F32)
    stream = residual_ref[...] + proj
    scale = lax.rsqrt(jnp.sum(stream * stream) * (1.0 / D) + 1e-05)
    normed = stream * scale * gain_ref[...]
    for i in range(BLOCKS):
        cols = slice(128 * i, 128 * i + 128)
        hidden_ref[0:1, cols] = stream[i : i + 1].astype(BF16)
        normed_ref[0:1, cols] = normed[i : i + 1].astype(BF16)


def local(
    query_new,
    key_new,
    value_new,
    prefix_keys,
    prefix_values,
    sample_suffix_keys,
    sample_suffix_values,
    prefix_len,
    suffix_len,
    residual,
    out_weight,
    norm_gain,
):
    place = lax.axis_index("mp").astype(jnp.int32)[None]
    cores = [[2 * z + c for z in range(CHIPS)] for c in range(2)]
    spread = pl.pallas_call(
        spread_kernel,
        out_shape=jax.ShapeDtypeStruct((SAMPLES, HQ, 128), BF16),
        in_specs=vmem(1),
        out_specs=vmem(1)[0],
        compiler_params=at_most(2),
        cost_estimate=LONG,
    )(query_new)
    queries = lax.all_to_all(spread, "mp", 0, 0, tiled=True)
    own, bias, residual_rows, gain_rows = pl.pallas_call(
        stage_kernel,
        out_shape=[
            jax.ShapeDtypeStruct((256, 1024), BF16),
            jax.ShapeDtypeStruct((2, 64, 128), F32),
            jax.ShapeDtypeStruct((BLOCKS, 128), F32),
            jax.ShapeDtypeStruct((BLOCKS, 128), F32),
        ],
        in_specs=smem(3) + vmem(6),
        out_specs=vmem(4),
        compiler_params=at_most(4),
        cost_estimate=LONG,
    )(
        place,
        prefix_len,
        suffix_len,
        sample_suffix_keys,
        sample_suffix_values,
        key_new,
        value_new,
        residual,
        norm_gain.reshape(BLOCKS, 128),
    )
    other_weight = lax.ppermute(out_weight, "mp", [(i, i ^ 1) for i in range(SAMPLES)])
    partial = pl.pallas_call(
        attend_kernel,
        out_shape=jax.ShapeDtypeStruct((SAMPLES, ROWS, 2, 128), BF16),
        in_specs=smem(1) + vmem(5),
        out_specs=vmem(1)[0],
        scratch_shapes=[pltpu.VMEM((SAMPLES * HQ, 128), F32)],
        compiler_params=at_most(8),
        cost_estimate=LONG,
    )(place, queries, prefix_keys, prefix_values, own, bias)
    partial = lax.all_to_all(partial, "mp", 0, 0, tiled=True)
    proj = pl.pallas_call(
        project_kernel,
        out_shape=jax.ShapeDtypeStruct((CHIPS, BLOCKS, 128), BF16),
        in_specs=smem(1) + vmem(2) + hbm(1),
        out_specs=vmem(1)[0],
        scratch_shapes=[
            pltpu.VMEM((8, D), F32),
            pltpu.VMEM((8 * BLOCKS, 128), F32),
            pltpu.VMEM((256, D), BF16),
            pltpu.SemaphoreType.DMA((D // WIDTH,)),
        ],
        compiler_params=at_most(16),
        cost_estimate=LONG,
    )(place, partial, out_weight, other_weight)
    proj = lax.all_to_all(proj, "mp", 0, 0, tiled=True, axis_index_groups=cores)
    return tuple(
        pl.pallas_call(
            finish_kernel,
            out_shape=[jax.ShapeDtypeStruct((1, D), BF16)] * 2,
            in_specs=vmem(3),
            out_specs=vmem(2),
            compiler_params=at_most(4),
        )(proj, residual_rows, gain_rows)
    )


def solution(mesh):
    whole = P(("dp", "mp"), None)
    placed = (
        whole,
        whole,
        whole,
        whole,
        whole,
        P(("dp", "mp"), None, None),
        P(("dp", "mp"), None, None),
        P("dp"),
        P(("dp", "mp")),
        whole,
        P("mp", None),
        P(),
    )

    def step(*arrays):
        return local(*arrays)

    step = jax.shard_map(
        step, mesh=mesh, in_specs=placed, out_specs=(whole, whole), check_vma=False
    )
    return step
```

```python
import jax
import jax.numpy as jnp
from jax import lax
from jax.experimental import pallas as pl
from jax.experimental.pallas import tpu as pltpu
from jax.sharding import PartitionSpec as P


HEAD_SIZE = 128
KEY_VALUE_HEADS = 8
HQ = 32
GROUP = HQ // KEY_VALUE_HEADS
SAMPLES = 16
CHIPS = 8
D = 8192
BLOCKS = D // 128
WIDTH = 1024
ROWS = 10
SCALE = HEAD_SIZE ** (-0.5)
MASKED = -1e30
LOWEST = -1e29
F32 = jnp.float32
BF16 = jnp.bfloat16

LONG = pl.CostEstimate(flops=10**10, bytes_accessed=10**6, transcendentals=0)


def vmem(count):
    return [pl.BlockSpec(memory_space=pltpu.VMEM)] * count


def at_most(mebibytes):
    return pltpu.CompilerParams(vmem_limit_bytes=mebibytes * 2**20)


def smem(count):
    return [pl.BlockSpec(memory_space=pltpu.SMEM)] * count


def spread_kernel(query_ref, out_ref):
    rows = [query_ref[0:1, h * 128 : (h + 1) * 128].astype(F32) for h in range(HQ)]
    rows = jnp.concatenate(rows, axis=0).astype(BF16)
    for i in range(CHIPS):
        out_ref[i] = rows


def pair_kernel(pkeys_ref, pvalues_ref, prefix_ref):
    prefix_ref[:128] = pkeys_ref[...]
    prefix_ref[128:] = pvalues_ref[...]


def stage_kernel(
    place_ref,
    prefix_len_ref,
    suffix_len_ref,
    skeys_ref,
    svalues_ref,
    key_ref,
    value_ref,
    residual_ref,
    gain_ref,
    own_ref,
    bias_ref,
    residual_rows_ref,
    gain_rows_ref,
):
    first = lax.broadcasted_iota(jnp.int32, (64, 1024), 0) == 0
    own_ref[0:64] = skeys_ref[0]
    own_ref[64:128] = jnp.where(first, key_ref[...].astype(F32), 0.0).astype(BF16)
    own_ref[128:192] = svalues_ref[0]
    own_ref[192:256] = jnp.where(first, value_ref[...].astype(F32), 0.0).astype(BF16)
    rows = [residual_ref[0:1, 128 * i : 128 * i + 128].astype(F32) for i in range(BLOCKS)]
    residual_rows_ref[...] = jnp.concatenate(rows, axis=0)
    gain_rows_ref[...] = gain_ref[...].astype(F32)
    place = place_ref[0]
    row = lax.broadcasted_iota(jnp.int32, (32, 128), 0)
    lane = lax.broadcasted_iota(jnp.int32, (32, 128), 1)
    prefix_len = prefix_len_ref[0]
    other_place = place + 1 - 2 * (place % 2)
    own = (row % 8 == place // 2) & ((lane < suffix_len_ref[0]) | (lane == 64))
    seen = (lane + place * 128 < prefix_len, lane + other_place * 128 < prefix_len, own)
    for i, mask in enumerate(seen):
        bias_ref[i] = jnp.where(mask, 0.0, MASKED)


def attend_kernel(
    place_ref,
    query_ref,
    prefix_ref,
    other_ref,
    own_ref,
    bias_ref,
    out_ref,
    queries,
):
    queries[...] = query_ref[...].reshape(CHIPS * HQ, 128).astype(F32)
    row = lax.broadcasted_iota(jnp.int32, (32, 128), 0)
    lane = lax.broadcasted_iota(jnp.int32, (32, 128), 1)
    mark = lane == row % 16 + 16 * (place_ref[0] // 2)
    ones = jnp.ones((384, 128), BF16)
    zeros = jnp.zeros((1, 128), F32)
    heads = [slice(k * 128, (k + 1) * 128) for k in range(KEY_VALUE_HEADS)]
    parts = (prefix_ref, other_ref, own_ref)
    scores = []
    for k, head in enumerate(heads):
        query = [queries[pl.ds(k * GROUP + g, 8, stride=HQ), :] for g in range(GROUP)]
        query = jnp.concatenate(query, axis=0).astype(BF16)
        keys = jnp.concatenate([part[:128, head] for part in parts], axis=0)
        product = lax.dot_general(
            query, keys, (((1,), (1,)), ((), ())), preferred_element_type=F32
        )
        scores.append(
            [product[:, 128 * i : 128 * i + 128] * SCALE + bias_ref[i] for i in range(3)]
        )
    tops = [jnp.maximum(jnp.maximum(s[0], s[1]), s[2]) for s in scores]
    tops = [jnp.max(top, axis=-1, keepdims=True) for top in tops]
    tops = [jnp.maximum(top, LOWEST).astype(BF16).astype(F32) for top in tops]
    weights = [
        jnp.concatenate([jnp.exp(s - top) for s in three], axis=1).astype(BF16)
        for three, top in zip(scores, tops)
    ]
    summed = []
    for weight, head in zip(weights, heads):
        values = jnp.concatenate([part[128:, head] for part in parts], axis=0)
        values = jnp.concatenate([values, ones], axis=1)
        summed.append(jnp.dot(weight, values, preferred_element_type=F32))
    for k, (top, sums) in enumerate(zip(tops, summed)):
        total_high = sums[:, 128:].astype(BF16).astype(F32)
        total_low = sums[:, 128:] - total_high
        for c in range(2):
            part = slice(16 * c, 16 * c + 16)
            out_ref[2 * k + c, 0:8] = sums[part, :128].astype(BF16).reshape(8, 2, 128)
            stats = [
                jnp.sum(jnp.where(mark[part], v[part], 0.0), axis=0, keepdims=True)
                for v in (top, total_high, total_low)
            ]
            stats = jnp.concatenate(stats + [zeros], axis=0).astype(BF16)
            out_ref[2 * k + c, 8:ROWS] = stats.reshape(2, 2, 128)


def project_kernel(place_ref, got_ref, weight_ref, out_ref, rows):
    row = lax.broadcasted_iota(jnp.int32, (16, 128), 0)
    lane = lax.broadcasted_iota(jnp.int32, (16, 128), 1)
    diagonal = lane % 16 == row
    joined = []
    for c in range(2):
        sources = range(c, SAMPLES, 2)
        stats = sum(got_ref[i, 8:ROWS].reshape(4, 128).astype(F32) for i in sources)
        tops, totals = stats[0:1], stats[1:2] + stats[2:3]
        top = tops
        for shift in (64, 32, 16):
            top = jnp.maximum(top, pltpu.roll(top, shift, 1))
        factors = jnp.exp(tops - top)
        total = factors * totals
        for shift in (64, 32, 16):
            total = total + pltpu.roll(total, shift, 1)
        mix = jnp.where(diagonal, factors / total, 0.0)
        high = mix.astype(BF16)
        low = (mix - high.astype(F32)).astype(BF16)
        sums = jnp.concatenate([got_ref[i, 0:8].reshape(16, 128) for i in sources], axis=0)
        both = jnp.dot(jnp.concatenate([high, low], axis=0), sums, preferred_element_type=F32)
        joined.append(both[:16] + both[16:])
    attn = [jnp.concatenate([a[8 * g : 8 * g + 8] for a in joined], axis=0) for g in range(2)]
    attn = jnp.concatenate(attn, axis=1).astype(BF16)
    for n in range(0, D, WIDTH):
        piece = jnp.dot(attn, weight_ref[:, n : n + WIDTH], preferred_element_type=F32)
        for i in range(WIDTH // 128):
            for c in range(2):
                rows[pl.ds(c * BLOCKS + n // 128 + i, 8, stride=2 * BLOCKS), :] = piece[
                    8 * c : 8 * c + 8, 128 * i : 128 * i + 128
                ]
    out_ref[...] = rows[...].astype(BF16).reshape(SAMPLES, BLOCKS, 128)


def finish_kernel(got_ref, residual_ref, gain_ref, hidden_ref, normed_ref):
    proj = got_ref[0].astype(F32)
    for i in range(1, SAMPLES):
        proj += got_ref[i].astype(F32)
    stream = residual_ref[...] + proj
    scale = lax.rsqrt(jnp.sum(stream * stream) * (1.0 / D) + 1e-05)
    normed = stream * scale * gain_ref[...]
    for i in range(BLOCKS):
        cols = slice(128 * i, 128 * i + 128)
        hidden_ref[0:1, cols] = stream[i : i + 1].astype(BF16)
        normed_ref[0:1, cols] = normed[i : i + 1].astype(BF16)


def local(
    query_new,
    key_new,
    value_new,
    prefix_keys,
    prefix_values,
    sample_suffix_keys,
    sample_suffix_values,
    prefix_len,
    suffix_len,
    residual,
    out_weight,
    norm_gain,
):
    place = lax.axis_index("mp").astype(jnp.int32)[None]
    cores = [[2 * z + c for z in range(CHIPS)] for c in range(2)]
    spread = pl.pallas_call(
        spread_kernel,
        out_shape=jax.ShapeDtypeStruct((CHIPS, HQ, 128), BF16),
        in_specs=vmem(1),
        out_specs=vmem(1)[0],
        compiler_params=at_most(2),
        cost_estimate=LONG,
    )(query_new)
    queries = lax.all_to_all(spread, "mp", 0, 0, tiled=True, axis_index_groups=cores)
    prefix = pl.pallas_call(
        pair_kernel,
        out_shape=jax.ShapeDtypeStruct((256, 1024), BF16),
        in_specs=vmem(2),
        out_specs=vmem(1)[0],
        compiler_params=at_most(2),
        cost_estimate=LONG,
    )(prefix_keys, prefix_values)
    other_prefix = lax.ppermute(prefix, "mp", [(i, i ^ 1) for i in range(SAMPLES)])
    own, bias, residual_rows, gain_rows = pl.pallas_call(
        stage_kernel,
        out_shape=[
            jax.ShapeDtypeStruct((256, 1024), BF16),
            jax.ShapeDtypeStruct((3, 32, 128), F32),
            jax.ShapeDtypeStruct((BLOCKS, 128), F32),
            jax.ShapeDtypeStruct((BLOCKS, 128), F32),
        ],
        in_specs=smem(3) + vmem(6),
        out_specs=vmem(4),
        compiler_params=at_most(4),
        cost_estimate=LONG,
    )(
        place,
        prefix_len,
        suffix_len,
        sample_suffix_keys,
        sample_suffix_values,
        key_new,
        value_new,
        residual,
        norm_gain.reshape(BLOCKS, 128),
    )
    partial = pl.pallas_call(
        attend_kernel,
        out_shape=jax.ShapeDtypeStruct((SAMPLES, ROWS, 2, 128), BF16),
        in_specs=smem(1) + vmem(5),
        out_specs=vmem(1)[0],
        scratch_shapes=[pltpu.VMEM((CHIPS * HQ, 128), F32)],
        compiler_params=at_most(8),
        cost_estimate=LONG,
    )(place, queries, prefix, other_prefix, own, bias)
    partial = lax.all_to_all(partial, "mp", 0, 0, tiled=True)
    proj = pl.pallas_call(
        project_kernel,
        out_shape=jax.ShapeDtypeStruct((SAMPLES, BLOCKS, 128), BF16),
        in_specs=smem(1) + vmem(2),
        out_specs=vmem(1)[0],
        scratch_shapes=[pltpu.VMEM((SAMPLES * BLOCKS, 128), F32)],
        compiler_params=at_most(12),
        cost_estimate=LONG,
    )(place, partial, out_weight)
    proj = lax.all_to_all(proj, "mp", 0, 0, tiled=True)
    return tuple(
        pl.pallas_call(
            finish_kernel,
            out_shape=[jax.ShapeDtypeStruct((1, D), BF16)] * 2,
            in_specs=vmem(3),
            out_specs=vmem(2),
            compiler_params=at_most(4),
        )(proj, residual_rows, gain_rows)
    )


def solution(mesh):
    whole = P(("dp", "mp"), None)
    placed = (
        whole,
        whole,
        whole,
        whole,
        whole,
        P(("dp", "mp"), None, None),
        P(("dp", "mp"), None, None),
        P("dp"),
        P(("dp", "mp")),
        whole,
        P("mp", None),
        P(),
    )

    def step(*arrays):
        return local(*arrays)

    step = jax.shard_map(
        step, mesh=mesh, in_specs=placed, out_specs=(whole, whole), check_vma=False
    )
    return step
```

```python
import jax
import jax.numpy as jnp
from jax import lax
from jax.experimental import pallas as pl
from jax.experimental.pallas import tpu as pltpu
from jax.sharding import PartitionSpec as P


HEAD_SIZE = 128
KEY_VALUE_HEADS = 8
HQ = 32
GROUP = HQ // KEY_VALUE_HEADS
SAMPLES = 16
CHIPS = 8
D = 8192
BLOCKS = D // 128
WIDTH = 1024
ROWS = 10
SCALE = HEAD_SIZE ** (-0.5)
MASKED = -1e30
LOWEST = -1e29
F32 = jnp.float32
BF16 = jnp.bfloat16

LONG = pl.CostEstimate(flops=10**10, bytes_accessed=10**6, transcendentals=0)


def vmem(count):
    return [pl.BlockSpec(memory_space=pltpu.VMEM)] * count


def at_most(mebibytes):
    return pltpu.CompilerParams(vmem_limit_bytes=mebibytes * 2**20)


def smem(count):
    return [pl.BlockSpec(memory_space=pltpu.SMEM)] * count


def spread_kernel(query_ref, out_ref):
    rows = [query_ref[0:1, h * 128 : (h + 1) * 128].astype(F32) for h in range(HQ)]
    rows = jnp.concatenate(rows, axis=0).astype(BF16)
    for i in range(CHIPS):
        out_ref[i] = rows


def pair_kernel(pkeys_ref, pvalues_ref, prefix_ref):
    prefix_ref[:128] = pkeys_ref[...]
    prefix_ref[128:] = pvalues_ref[...]


def stage_kernel(
    place_ref,
    prefix_len_ref,
    suffix_len_ref,
    skeys_ref,
    svalues_ref,
    key_ref,
    value_ref,
    residual_ref,
    gain_ref,
    own_ref,
    bias_ref,
    residual_rows_ref,
    gain_rows_ref,
):
    first = lax.broadcasted_iota(jnp.int32, (64, 1024), 0) == 0
    own_ref[0:64] = skeys_ref[0]
    own_ref[64:128] = jnp.where(first, key_ref[...].astype(F32), 0.0).astype(BF16)
    own_ref[128:192] = svalues_ref[0]
    own_ref[192:256] = jnp.where(first, value_ref[...].astype(F32), 0.0).astype(BF16)
    rows = [residual_ref[0:1, 128 * i : 128 * i + 128].astype(F32) for i in range(BLOCKS)]
    residual_rows_ref[...] = jnp.concatenate(rows, axis=0)
    gain_rows_ref[...] = gain_ref[...].astype(F32)
    place = place_ref[0]
    row = lax.broadcasted_iota(jnp.int32, (32, 128), 0)
    lane = lax.broadcasted_iota(jnp.int32, (32, 128), 1)
    prefix_len = prefix_len_ref[0]
    other_place = place + 1 - 2 * (place % 2)
    own = (row % 8 == place // 2) & ((lane < suffix_len_ref[0]) | (lane == 64))
    seen = (lane + place * 128 < prefix_len, lane + other_place * 128 < prefix_len, own)
    for i, mask in enumerate(seen):
        bias_ref[i] = jnp.where(mask, 0.0, MASKED)


def attend_kernel(
    place_ref,
    query_ref,
    prefix_ref,
    other_ref,
    own_ref,
    bias_ref,
    out_ref,
    queries,
):
    queries[...] = query_ref[...].reshape(CHIPS * HQ, 128).astype(F32)
    row = lax.broadcasted_iota(jnp.int32, (32, 128), 0)
    lane = lax.broadcasted_iota(jnp.int32, (32, 128), 1)
    mark = lane == row % 16 + 16 * (place_ref[0] // 2)
    ones = jnp.ones((384, 128), BF16)
    zeros = jnp.zeros((1, 128), F32)
    heads = [slice(k * 128, (k + 1) * 128) for k in range(KEY_VALUE_HEADS)]
    parts = (prefix_ref, other_ref, own_ref)
    scores = []
    for k, head in enumerate(heads):
        query = [queries[pl.ds(k * GROUP + g, 8, stride=HQ), :] for g in range(GROUP)]
        query = jnp.concatenate(query, axis=0).astype(BF16)
        keys = jnp.concatenate([part[:128, head] for part in parts], axis=0)
        product = lax.dot_general(
            query, keys, (((1,), (1,)), ((), ())), preferred_element_type=F32
        )
        scores.append(
            [product[:, 128 * i : 128 * i + 128] * SCALE + bias_ref[i] for i in range(3)]
        )
    tops = [jnp.maximum(jnp.maximum(s[0], s[1]), s[2]) for s in scores]
    tops = [jnp.max(top, axis=-1, keepdims=True) for top in tops]
    tops = [jnp.maximum(top, LOWEST).astype(BF16).astype(F32) for top in tops]
    weights = [
        jnp.concatenate([jnp.exp(s - top) for s in three], axis=1).astype(BF16)
        for three, top in zip(scores, tops)
    ]
    summed = []
    for weight, head in zip(weights, heads):
        values = jnp.concatenate([part[128:, head] for part in parts], axis=0)
        values = jnp.concatenate([values, ones], axis=1)
        summed.append(jnp.dot(weight, values, preferred_element_type=F32))
    for k, (top, sums) in enumerate(zip(tops, summed)):
        total_high = sums[:, 128:].astype(BF16).astype(F32)
        total_low = sums[:, 128:] - total_high
        for c in range(2):
            part = slice(16 * c, 16 * c + 16)
            out_ref[2 * k + c, 0:8] = sums[part, :128].astype(BF16).reshape(8, 2, 128)
            stats = [
                jnp.sum(jnp.where(mark[part], v[part], 0.0), axis=0, keepdims=True)
                for v in (top, total_high, total_low)
            ]
            stats = jnp.concatenate(stats + [zeros], axis=0).astype(BF16)
            out_ref[2 * k + c, 8:ROWS] = stats.reshape(2, 2, 128)


def project_kernel(place_ref, got_ref, weight_ref, out_ref, rows):
    row = lax.broadcasted_iota(jnp.int32, (16, 128), 0)
    lane = lax.broadcasted_iota(jnp.int32, (16, 128), 1)
    diagonal = lane % 16 == row
    stats = [
        sum(got_ref[i, 8:ROWS].reshape(4, 128).astype(F32) for i in range(c, SAMPLES, 2))
        for c in range(2)
    ]
    tops = jnp.concatenate([s[0:1] for s in stats], axis=0)
    totals = jnp.concatenate([s[1:2] + s[2:3] for s in stats], axis=0)
    top = tops
    for shift in (64, 32, 16):
        top = jnp.maximum(top, pltpu.roll(top, shift, 1))
    factors = jnp.exp(tops - top)
    total = factors * totals
    for shift in (64, 32, 16):
        total = total + pltpu.roll(total, shift, 1)
    factors = factors / total
    mixes = [jnp.where(diagonal, factors[c : c + 1], 0.0) for c in range(2)]
    highs = [mix.astype(BF16) for mix in mixes]
    lows = [(mix - high.astype(F32)).astype(BF16) for mix, high in zip(mixes, highs)]
    joined = []
    for c in range(2):
        sums = [got_ref[i, 0:8].reshape(16, 128) for i in range(c, SAMPLES, 2)]
        sums = jnp.concatenate(sums, axis=0)
        both = jnp.concatenate([highs[c], lows[c]], axis=0)
        joined.append(jnp.dot(both, sums, preferred_element_type=F32))
    joined = [both[:16] + both[16:] for both in joined]
    attn = [jnp.concatenate([a[8 * g : 8 * g + 8] for a in joined], axis=0) for g in range(2)]
    attn = jnp.concatenate(attn, axis=1).astype(BF16)
    for n in range(0, D, WIDTH):
        piece = jnp.dot(attn, weight_ref[:, n : n + WIDTH], preferred_element_type=F32)
        for i in range(WIDTH // 128):
            for c in range(2):
                rows[pl.ds(c * BLOCKS + n // 128 + i, 8, stride=2 * BLOCKS), :] = piece[
                    8 * c : 8 * c + 8, 128 * i : 128 * i + 128
                ]
    out_ref[...] = rows[...].astype(BF16).reshape(SAMPLES, BLOCKS, 128)


def finish_kernel(got_ref, residual_ref, gain_ref, hidden_ref, normed_ref):
    proj = got_ref[0].astype(F32)
    for i in range(1, SAMPLES):
        proj += got_ref[i].astype(F32)
    stream = residual_ref[...] + proj
    scale = lax.rsqrt(jnp.sum(stream * stream) * (1.0 / D) + 1e-05)
    normed = stream * scale * gain_ref[...]
    for i in range(BLOCKS):
        cols = slice(128 * i, 128 * i + 128)
        hidden_ref[0:1, cols] = stream[i : i + 1].astype(BF16)
        normed_ref[0:1, cols] = normed[i : i + 1].astype(BF16)


def local(
    query_new,
    key_new,
    value_new,
    prefix_keys,
    prefix_values,
    sample_suffix_keys,
    sample_suffix_values,
    prefix_len,
    suffix_len,
    residual,
    out_weight,
    norm_gain,
):
    place = lax.axis_index("mp").astype(jnp.int32)[None]
    cores = [[2 * z + c for z in range(CHIPS)] for c in range(2)]
    spread = pl.pallas_call(
        spread_kernel,
        out_shape=jax.ShapeDtypeStruct((CHIPS, HQ, 128), BF16),
        in_specs=vmem(1),
        out_specs=vmem(1)[0],
        compiler_params=at_most(2),
        cost_estimate=LONG,
    )(query_new)
    queries = lax.all_to_all(spread, "mp", 0, 0, tiled=True, axis_index_groups=cores)
    prefix = pl.pallas_call(
        pair_kernel,
        out_shape=jax.ShapeDtypeStruct((256, 1024), BF16),
        in_specs=vmem(2),
        out_specs=vmem(1)[0],
        compiler_params=at_most(2),
        cost_estimate=LONG,
    )(prefix_keys, prefix_values)
    other_prefix = lax.ppermute(prefix, "mp", [(i, i ^ 1) for i in range(SAMPLES)])
    own, bias, residual_rows, gain_rows = pl.pallas_call(
        stage_kernel,
        out_shape=[
            jax.ShapeDtypeStruct((256, 1024), BF16),
            jax.ShapeDtypeStruct((3, 32, 128), F32),
            jax.ShapeDtypeStruct((BLOCKS, 128), F32),
            jax.ShapeDtypeStruct((BLOCKS, 128), F32),
        ],
        in_specs=smem(3) + vmem(6),
        out_specs=vmem(4),
        compiler_params=at_most(4),
        cost_estimate=LONG,
    )(
        place,
        prefix_len,
        suffix_len,
        sample_suffix_keys,
        sample_suffix_values,
        key_new,
        value_new,
        residual,
        norm_gain.reshape(BLOCKS, 128),
    )
    partial = pl.pallas_call(
        attend_kernel,
        out_shape=jax.ShapeDtypeStruct((SAMPLES, ROWS, 2, 128), BF16),
        in_specs=smem(1) + vmem(5),
        out_specs=vmem(1)[0],
        scratch_shapes=[pltpu.VMEM((CHIPS * HQ, 128), F32)],
        compiler_params=at_most(8),
        cost_estimate=LONG,
    )(place, queries, prefix, other_prefix, own, bias)
    partial = lax.all_to_all(partial, "mp", 0, 0, tiled=True)
    proj = pl.pallas_call(
        project_kernel,
        out_shape=jax.ShapeDtypeStruct((SAMPLES, BLOCKS, 128), BF16),
        in_specs=smem(1) + vmem(2),
        out_specs=vmem(1)[0],
        scratch_shapes=[pltpu.VMEM((SAMPLES * BLOCKS, 128), F32)],
        compiler_params=at_most(12),
        cost_estimate=LONG,
    )(place, partial, out_weight)
    proj = lax.all_to_all(proj, "mp", 0, 0, tiled=True)
    return tuple(
        pl.pallas_call(
            finish_kernel,
            out_shape=[jax.ShapeDtypeStruct((1, D), BF16)] * 2,
            in_specs=vmem(3),
            out_specs=vmem(2),
            compiler_params=at_most(4),
        )(proj, residual_rows, gain_rows)
    )


def solution(mesh):
    whole = P(("dp", "mp"), None)
    placed = (
        whole,
        whole,
        whole,
        whole,
        whole,
        P(("dp", "mp"), None, None),
        P(("dp", "mp"), None, None),
        P("dp"),
        P(("dp", "mp")),
        whole,
        P("mp", None),
        P(),
    )

    def step(*arrays):
        return local(*arrays)

    step = jax.shard_map(
        step, mesh=mesh, in_specs=placed, out_specs=(whole, whole), check_vma=False
    )
    return step
```

```python
import jax
import jax.numpy as jnp
from jax import lax
from jax.experimental import pallas as pl
from jax.experimental.pallas import tpu as pltpu
from jax.sharding import PartitionSpec as P


HEAD_SIZE = 128
KEY_VALUE_HEADS = 8
HQ = 32
GROUP = HQ // KEY_VALUE_HEADS
SAMPLES = 16
CHIPS = 8
D = 8192
BLOCKS = D // 128
PITCH = BLOCKS + 8
QUERY_PITCH = HQ + 8
WIDTH = 1024
ROWS = 10
SCALE = HEAD_SIZE ** (-0.5)
MASKED = -1e30
LOWEST = -1e29
F32 = jnp.float32
BF16 = jnp.bfloat16

LONG = pl.CostEstimate(flops=10**10, bytes_accessed=10**6, transcendentals=0)


def vmem(count):
    return [pl.BlockSpec(memory_space=pltpu.VMEM)] * count


def at_most(mebibytes):
    return pltpu.CompilerParams(vmem_limit_bytes=mebibytes * 2**20)


def smem(count):
    return [pl.BlockSpec(memory_space=pltpu.SMEM)] * count


def spread_kernel(query_ref, out_ref):
    rows = [query_ref[0:1, h * 128 : (h + 1) * 128].astype(F32) for h in range(HQ)]
    rows = jnp.concatenate(rows, axis=0).astype(BF16)
    for i in range(CHIPS):
        out_ref[i] = rows


def pair_kernel(pkeys_ref, pvalues_ref, prefix_ref):
    prefix_ref[:128] = pkeys_ref[...]
    prefix_ref[128:] = pvalues_ref[...]


def stage_kernel(
    place_ref,
    prefix_len_ref,
    suffix_len_ref,
    skeys_ref,
    svalues_ref,
    key_ref,
    value_ref,
    residual_ref,
    gain_ref,
    own_ref,
    bias_ref,
    residual_rows_ref,
    gain_rows_ref,
):
    first = lax.broadcasted_iota(jnp.int32, (64, 1024), 0) == 0
    own_ref[0:64] = skeys_ref[0]
    own_ref[64:128] = jnp.where(first, key_ref[...].astype(F32), 0.0).astype(BF16)
    own_ref[128:192] = svalues_ref[0]
    own_ref[192:256] = jnp.where(first, value_ref[...].astype(F32), 0.0).astype(BF16)
    rows = [residual_ref[0:1, 128 * i : 128 * i + 128].astype(F32) for i in range(BLOCKS)]
    residual_rows_ref[...] = jnp.concatenate(rows, axis=0)
    gain_rows_ref[...] = gain_ref[...].astype(F32)
    place = place_ref[0]
    row = lax.broadcasted_iota(jnp.int32, (32, 128), 0)
    lane = lax.broadcasted_iota(jnp.int32, (32, 128), 1)
    prefix_len = prefix_len_ref[0]
    other_place = place + 1 - 2 * (place % 2)
    own = (row % 8 == place // 2) & ((lane < suffix_len_ref[0]) | (lane == 64))
    seen = (lane + place * 128 < prefix_len, lane + other_place * 128 < prefix_len, own)
    for i, mask in enumerate(seen):
        bias_ref[i] = jnp.where(mask, 0.0, MASKED)


def attend_kernel(
    place_ref,
    query_ref,
    prefix_ref,
    other_ref,
    own_ref,
    bias_ref,
    out_ref,
    queries,
):
    for i in range(CHIPS):
        queries[QUERY_PITCH * i : QUERY_PITCH * i + HQ] = query_ref[i].astype(F32)
    row = lax.broadcasted_iota(jnp.int32, (32, 128), 0)
    lane = lax.broadcasted_iota(jnp.int32, (32, 128), 1)
    mark = lane == row % 16 + 16 * (place_ref[0] // 2)
    ones = jnp.ones((384, 128), BF16)
    zeros = jnp.zeros((1, 128), F32)
    heads = [slice(k * 128, (k + 1) * 128) for k in range(KEY_VALUE_HEADS)]
    parts = (prefix_ref, other_ref, own_ref)
    scores = []
    for k, head in enumerate(heads):
        query = [queries[pl.ds(k * GROUP + g, 8, stride=QUERY_PITCH), :] for g in range(GROUP)]
        query = jnp.concatenate(query, axis=0).astype(BF16)
        keys = jnp.concatenate([part[:128, head] for part in parts], axis=0)
        product = lax.dot_general(
            query, keys, (((1,), (1,)), ((), ())), preferred_element_type=F32
        )
        scores.append(
            [product[:, 128 * i : 128 * i + 128] * SCALE + bias_ref[i] for i in range(3)]
        )
    tops = [jnp.maximum(jnp.maximum(s[0], s[1]), s[2]) for s in scores]
    tops = [jnp.max(top, axis=-1, keepdims=True) for top in tops]
    tops = [jnp.maximum(top, LOWEST).astype(BF16).astype(F32) for top in tops]
    weights = [
        jnp.concatenate([jnp.exp(s - top) for s in three], axis=1).astype(BF16)
        for three, top in zip(scores, tops)
    ]
    summed = []
    for weight, head in zip(weights, heads):
        values = jnp.concatenate([part[128:, head] for part in parts], axis=0)
        values = jnp.concatenate([values, ones], axis=1)
        summed.append(jnp.dot(weight, values, preferred_element_type=F32))
    for k, (top, sums) in enumerate(zip(tops, summed)):
        total_high = sums[:, 128:].astype(BF16).astype(F32)
        total_low = sums[:, 128:] - total_high
        for c in range(2):
            part = slice(16 * c, 16 * c + 16)
            out_ref[2 * k + c, 0:8] = sums[part, :128].astype(BF16).reshape(8, 2, 128)
            stats = [
                jnp.sum(jnp.where(mark[part], v[part], 0.0), axis=0, keepdims=True)
                for v in (top, total_high, total_low)
            ]
            stats = jnp.concatenate(stats + [zeros], axis=0).astype(BF16)
            out_ref[2 * k + c, 8:ROWS] = stats.reshape(2, 2, 128)


def project_kernel(place_ref, got_ref, weight_ref, out_ref, rows):
    row = lax.broadcasted_iota(jnp.int32, (16, 128), 0)
    lane = lax.broadcasted_iota(jnp.int32, (16, 128), 1)
    diagonal = lane % 16 == row
    stats = [
        sum(got_ref[i, 8:ROWS].reshape(4, 128).astype(F32) for i in range(c, SAMPLES, 2))
        for c in range(2)
    ]
    tops = jnp.concatenate([s[0:1] for s in stats], axis=0)
    totals = jnp.concatenate([s[1:2] + s[2:3] for s in stats], axis=0)
    top = tops
    for shift in (64, 32, 16):
        top = jnp.maximum(top, pltpu.roll(top, shift, 1))
    factors = jnp.exp(tops - top)
    total = factors * totals
    for shift in (64, 32, 16):
        total = total + pltpu.roll(total, shift, 1)
    factors = factors / total
    mixes = [jnp.where(diagonal, factors[c : c + 1], 0.0) for c in range(2)]
    highs = [mix.astype(BF16) for mix in mixes]
    lows = [(mix - high.astype(F32)).astype(BF16) for mix, high in zip(mixes, highs)]
    joined = []
    for c in range(2):
        sums = [got_ref[i, 0:8].reshape(16, 128) for i in range(c, SAMPLES, 2)]
        sums = jnp.concatenate(sums, axis=0)
        both = jnp.concatenate([highs[c], lows[c]], axis=0)
        joined.append(jnp.dot(both, sums, preferred_element_type=F32))
    joined = [both[:16] + both[16:] for both in joined]
    attn = [jnp.concatenate([a[8 * g : 8 * g + 8] for a in joined], axis=0) for g in range(2)]
    attn = jnp.concatenate(attn, axis=1).astype(BF16)
    for n in range(0, D, WIDTH):
        piece = jnp.dot(attn, weight_ref[:, n : n + WIDTH], preferred_element_type=F32)
        for i in range(WIDTH // 128):
            for c in range(2):
                rows[pl.ds(8 * PITCH * c + n // 128 + i, 8, stride=PITCH), :] = piece[
                    8 * c : 8 * c + 8, 128 * i : 128 * i + 128
                ]
    for b in range(SAMPLES):
        at = PITCH * (8 * (b % 2) + b // 2)
        out_ref[b] = rows[at : at + BLOCKS].astype(BF16)


def finish_kernel(got_ref, residual_ref, gain_ref, hidden_ref, normed_ref):
    proj = got_ref[0].astype(F32)
    for i in range(1, SAMPLES):
        proj += got_ref[i].astype(F32)
    stream = residual_ref[...] + proj
    scale = lax.rsqrt(jnp.sum(stream * stream) * (1.0 / D) + 1e-05)
    normed = stream * scale * gain_ref[...]
    for i in range(BLOCKS):
        cols = slice(128 * i, 128 * i + 128)
        hidden_ref[0:1, cols] = stream[i : i + 1].astype(BF16)
        normed_ref[0:1, cols] = normed[i : i + 1].astype(BF16)


def local(
    query_new,
    key_new,
    value_new,
    prefix_keys,
    prefix_values,
    sample_suffix_keys,
    sample_suffix_values,
    prefix_len,
    suffix_len,
    residual,
    out_weight,
    norm_gain,
):
    place = lax.axis_index("mp").astype(jnp.int32)[None]
    cores = [[2 * z + c for z in range(CHIPS)] for c in range(2)]
    spread = pl.pallas_call(
        spread_kernel,
        out_shape=jax.ShapeDtypeStruct((CHIPS, HQ, 128), BF16),
        in_specs=vmem(1),
        out_specs=vmem(1)[0],
        compiler_params=at_most(2),
        cost_estimate=LONG,
    )(query_new)
    queries = lax.all_to_all(spread, "mp", 0, 0, tiled=True, axis_index_groups=cores)
    prefix = pl.pallas_call(
        pair_kernel,
        out_shape=jax.ShapeDtypeStruct((256, 1024), BF16),
        in_specs=vmem(2),
        out_specs=vmem(1)[0],
        compiler_params=at_most(2),
        cost_estimate=LONG,
    )(prefix_keys, prefix_values)
    other_prefix = lax.ppermute(prefix, "mp", [(i, i ^ 1) for i in range(SAMPLES)])
    own, bias, residual_rows, gain_rows = pl.pallas_call(
        stage_kernel,
        out_shape=[
            jax.ShapeDtypeStruct((256, 1024), BF16),
            jax.ShapeDtypeStruct((3, 32, 128), F32),
            jax.ShapeDtypeStruct((BLOCKS, 128), F32),
            jax.ShapeDtypeStruct((BLOCKS, 128), F32),
        ],
        in_specs=smem(3) + vmem(6),
        out_specs=vmem(4),
        compiler_params=at_most(4),
        cost_estimate=LONG,
    )(
        place,
        prefix_len,
        suffix_len,
        sample_suffix_keys,
        sample_suffix_values,
        key_new,
        value_new,
        residual,
        norm_gain.reshape(BLOCKS, 128),
    )
    partial = pl.pallas_call(
        attend_kernel,
        out_shape=jax.ShapeDtypeStruct((SAMPLES, ROWS, 2, 128), BF16),
        in_specs=smem(1) + vmem(5),
        out_specs=vmem(1)[0],
        scratch_shapes=[pltpu.VMEM((CHIPS * QUERY_PITCH, 128), F32)],
        compiler_params=at_most(8),
        cost_estimate=LONG,
    )(place, queries, prefix, other_prefix, own, bias)
    partial = lax.all_to_all(partial, "mp", 0, 0, tiled=True)
    proj = pl.pallas_call(
        project_kernel,
        out_shape=jax.ShapeDtypeStruct((SAMPLES, BLOCKS, 128), BF16),
        in_specs=smem(1) + vmem(2),
        out_specs=vmem(1)[0],
        scratch_shapes=[pltpu.VMEM((SAMPLES * PITCH, 128), F32)],
        compiler_params=at_most(12),
        cost_estimate=LONG,
    )(place, partial, out_weight)
    proj = lax.all_to_all(proj, "mp", 0, 0, tiled=True)
    return tuple(
        pl.pallas_call(
            finish_kernel,
            out_shape=[jax.ShapeDtypeStruct((1, D), BF16)] * 2,
            in_specs=vmem(3),
            out_specs=vmem(2),
            compiler_params=at_most(4),
        )(proj, residual_rows, gain_rows)
    )


def solution(mesh):
    whole = P(("dp", "mp"), None)
    placed = (
        whole,
        whole,
        whole,
        whole,
        whole,
        P(("dp", "mp"), None, None),
        P(("dp", "mp"), None, None),
        P("dp"),
        P(("dp", "mp")),
        whole,
        P("mp", None),
        P(),
    )

    def step(*arrays):
        return local(*arrays)

    step = jax.shard_map(
        step, mesh=mesh, in_specs=placed, out_specs=(whole, whole), check_vma=False
    )
    return step
```
